32 devices in a mesh: dp: 4 (over y, x), expert: 8 (over z, core).
Axes of the slice: x: 2, y: 2, z: 4, core: 2. Of those that a mesh axis runs over, the one named last changes fastest.
Arguments:
- out_grad: bfloat16 [384, 3072], P(('dp', 'expert')), may hold values from -6 to 6
- layer_input: bfloat16 [384, 3072], P(('dp', 'expert')), may hold values from -6 to 6
- expert_ids: int32 [384, 2], P(('dp', 'expert')), may hold values from 0 to 7, as said below
- gate_prob: float32 [384, 2], P(('dp', 'expert')), may hold values from 0.05 to 1
- w_stack: bfloat16 [3, 3072, 8192], P(None, 'dp', 'expert'), may hold values from -0.109375 to 0.109375
- scale_exps: int32 [3, 24, 64], P(None, 'dp', 'expert'), may hold values from -1 to 1
Outputs:
- input_grad: bfloat16 [384, 3072], P(('dp', 'expert'))
- weight_grads: float32 [3, 3072, 8192], P(None, 'dp', 'expert')
The draws below stay inside these ranges and needn't reach their ends.
Inputs may be any that keep to these rules, and one draw needn't show every extreme that they name: `expert_ids`: each row names two different experts. In each aligned block of 12 rows (the tokens of one device) between 1 and 3 rows name expert 0, and some blocks have exactly 3 in every draw.
All inputs are finite; a program needn't handle non-finite values.
Results may differ from the reference program's by a relative error of at most 0.015.
Values may be sent and summed in bfloat16 or wider, within the bound.
No kernel may reach another device: no remote copies, remote signals or barrier semaphores. Data moves between devices by JAX's collectives and lax.ppermute only.
A program may use at most 128 MiB of HBM per device.

```python
import math
import jax
import jax.numpy as jnp
from jax import lax

D = 3072
FF = 8192
EXPERTS = 8
TOP = 2
TILE = 128
CAP = 3
TOK_DEV = 12
TOKENS = 384
N_DP = 4
N_EXPERT = 8


def draw_expert_ids(key, part):
    block_count = TOKENS // TOK_DEV
    subkeys = jax.random.split(jax.random.fold_in(key, 11), 7)
    counts = jax.random.randint(subkeys[0], (block_count,), 1, CAP + 1)
    full_block = jax.random.randint(subkeys[1], (block_count,), 0, 4) == 0
    chosen = jax.random.randint(subkeys[2], (), 0, block_count)
    counts = jnp.where(full_block | (jnp.arange(block_count) == chosen), CAP, counts)
    ranks = jax.vmap(lambda subkey: jax.random.permutation(subkey, TOK_DEV))(jax.random.split(subkeys[3], block_count))
    routed = ranks < counts[:, None]
    first_pick = jax.random.randint(subkeys[4], (block_count, TOK_DEV), 1, EXPERTS)
    offset = jax.random.randint(subkeys[5], (block_count, TOK_DEV), 1, EXPERTS - 1)
    second = 1 + (first_pick - 1 + offset) % (EXPERTS - 1)
    flipped = jax.random.randint(subkeys[6], (block_count, TOK_DEV), 0, 2) == 1
    column_left = jnp.where(routed, jnp.where(flipped, first_pick, 0), first_pick)
    column_right = jnp.where(routed, jnp.where(flipped, 0, first_pick), second)
    return jnp.stack([column_left, column_right], axis=-1).reshape(TOKENS, 2).astype(jnp.int32)


def with_ends(entries, stream_key, low, high):
    longest = entries.shape.index(max(entries.shape))
    spots = []
    for shift in (0, 1):
        where = [jax.random.randint(jax.random.fold_in(stream_key, axis), (), 0, length) for axis, length in enumerate(entries.shape)]
        where[longest] = (where[longest] + shift) % entries.shape[longest]
        spots.append(tuple(where))
    return entries.at[spots[0]].set(low).at[spots[1]].set(high)


def levels(rng, shape, cuts, low, high):
    def one(axis_at, parts):
        steps = jax.random.uniform(jax.random.fold_in(jax.random.fold_in(rng, 6), axis_at), (parts,), jnp.float32, low / len(cuts), high / len(cuts))
        return jnp.repeat(jnp.exp(steps), shape[axis_at] // parts).reshape((-1,) + (1,) * (len(shape) - axis_at - 1))

    loudness = one(*cuts[0])
    for cut in cuts[1:]:
        loudness = loudness * one(*cut)
    return loudness


def scatter_about(stream_key, dims, deviation, limit, pieces=(), kind=jnp.bfloat16):
    drawn = jax.random.normal(stream_key, dims, jnp.float32) * deviation
    if len(pieces) > 0:
        drawn = levels(stream_key, dims, pieces, -0.22, 0.18) * drawn
    return jnp.clip(drawn, min=-limit, max=limit).astype(kind)


def setup_inputs(seed: int = 0) -> dict:
    key_list = jax.random.split(jax.random.key(seed), 7)
    return {
        "out_grad": scatter_about(key_list[0], (TOKENS, D), 1.0, 6.0, ((0, 32),)),
        "layer_input": scatter_about(key_list[1], (TOKENS, D), 1.0, 6.0, ((0, 32),)),
        "expert_ids": draw_expert_ids(jax.random.fold_in(key_list[6], 71), 0),
        "gate_prob": jnp.clip(jnp.exp(math.log(1.0) - 2.9957323 * jax.random.uniform(key_list[3], (TOKENS, TOP), jnp.float32) ** levels(key_list[3], (TOKENS, TOP), ((0, 32),), -0.2, 0.2)), 0.05, 1.0),
        "w_stack": scatter_about(key_list[4], (3, D, FF), D ** -0.5, 0.109375, ((1, 4), (2, 8))),
        "scale_exps": with_ends(jax.random.randint(key_list[5], (3, D // TILE, FF // TILE), -1, 2), jax.random.fold_in(key_list[5], 1), -1, 1).astype(jnp.int32),
    }


def dequantize(w_stack, scale_exps):
    factor = jnp.exp2(scale_exps.astype(jnp.float32))
    scaled = w_stack.astype(jnp.float32).reshape(3, D // TILE, TILE, FF // TILE, TILE) * factor[:, :, None, :, None]
    return scaled.reshape(3, D, FF).astype(jnp.bfloat16)


def contract_rows(left, right):
    return lax.dot_general(left, right, (((0,), (0,)), ((), ())), preferred_element_type=jnp.float32)


def back_project(grad_rows, matrix):
    return lax.dot_general(grad_rows, matrix, (((1,), (1,)), ((), ())), preferred_element_type=jnp.float32)


def expert_backward(routed_input, routed_grad, weights):
    gate_value = jnp.dot(routed_input, weights[0], preferred_element_type=jnp.float32)
    up_value = jnp.dot(routed_input, weights[1], preferred_element_type=jnp.float32)
    down_back = jnp.dot(routed_grad, weights[2], preferred_element_type=jnp.float32)
    gate_sigmoid = jax.nn.sigmoid(gate_value)
    gate_act = gate_value * gate_sigmoid
    gate_grad = (down_back * up_value * gate_sigmoid * (1.0 + gate_value * (1.0 - gate_sigmoid))).astype(jnp.bfloat16)
    up_grad = (down_back * gate_act).astype(jnp.bfloat16)
    hidden = (gate_act * up_value).astype(jnp.bfloat16)
    returned = back_project(gate_grad, weights[0]) + back_project(up_grad, weights[1])
    partial_value = jnp.stack([contract_rows(routed_input, gate_grad), contract_rows(routed_input, up_grad), contract_rows(routed_grad, hidden)])
    return returned, partial_value


def reference(out_grad, layer_input, expert_ids, gate_prob, w_stack, scale_exps):
    weights = dequantize(w_stack, scale_exps)
    routed = expert_ids == 0
    routed_mask = jnp.any(routed, axis=1)
    expert_prob = jnp.sum(jnp.where(routed, gate_prob, 0.0), axis=1)
    block_count = out_grad.shape[0] // TOK_DEV
    block_mask = routed_mask.reshape(block_count, TOK_DEV)
    slot_index = jnp.cumsum(block_mask.astype(jnp.int32), axis=1) - 1
    places = jnp.arange(CAP, dtype=jnp.int32)
    slot_hit = (slot_index[:, None, :] == places[None, :, None]) & block_mask[:, None, :]
    positions = jnp.arange(TOK_DEV, dtype=jnp.int32)
    source = jnp.sum(jnp.where(slot_hit, positions[None, None, :], 0), axis=2)
    source = (source + (jnp.arange(block_count, dtype=jnp.int32) * TOK_DEV)[:, None]).reshape(-1)
    slot_valid = jnp.any(slot_hit, axis=2).reshape(-1)
    slot_input = jnp.where(slot_valid[:, None], layer_input[source], jnp.zeros((), jnp.bfloat16))
    slot_grad = jnp.where(slot_valid[:, None], expert_prob[source][:, None] * out_grad[source].astype(jnp.float32), 0.0).astype(jnp.bfloat16)
    slot_rows = N_EXPERT * CAP
    group_input = slot_input.reshape(N_DP, slot_rows, D)
    group_grad = slot_grad.reshape(N_DP, slot_rows, D)

    def group_step(total, pair):
        returned, partial_value = expert_backward(pair[0], pair[1], weights)
        rounded = lax.optimization_barrier(partial_value.astype(jnp.bfloat16))
        return total + rounded.astype(jnp.float32), returned

    weight_grads, returned = lax.scan(group_step, jnp.zeros((3, D, FF), jnp.float32), (group_input, group_grad))
    returned = returned.reshape(block_count, CAP, D)
    picked = jnp.take_along_axis(returned, jnp.clip(slot_index, 0, CAP - 1)[:, :, None], axis=1)
    input_grad = jnp.where(block_mask[:, :, None], picked, 0.0).reshape(-1, D).astype(jnp.bfloat16)
    return input_grad, weight_grads
```

```python
import jax
import jax.numpy as jnp
from jax import lax
from jax.experimental import pallas as pl
from jax.experimental.pallas import tpu as pltpu
from jax.sharding import PartitionSpec as P

CAP = 3
BF16 = jnp.bfloat16
F32 = jnp.float32
I32 = jnp.int32
ROWS = 8
CORES = 2
VMEM = pltpu.VMEM
SMEM = pltpu.SMEM


def log2(n):
    return n.bit_length() - 1


def is_pow2(n):
    return n & (n - 1) == 0


def xor_pairs(n, k):
    return [(i, i ^ k) for i in range(n)]


def nn(a, b):
    return lax.dot_general(a, b, (((1,), (0,)), ((), ())), preferred_element_type=F32)


def nt(a, b):
    return lax.dot_general(a, b, (((1,), (1,)), ((), ())), preferred_element_type=F32)


def tn(a, b):
    return lax.dot_general(a, b, (((0,), (0,)), ((), ())), preferred_element_type=F32)


def slots_kernel(p_ref, ids_ref, prob_ref, grad_ref, inp_ref, hit_ref, *refs):
    outs, scratch = refs[:-1], refs[-1]
    n_dp = len(outs)
    width = outs[0].shape[1]
    tok = ids_ref.shape[1]
    named = ids_ref[...] == 0
    prob = jnp.sum(jnp.where(named, prob_ref[...], 0.0), axis=0, keepdims=True)
    routed = jnp.sum(named.astype(F32), axis=0, keepdims=True)
    earlier = lax.broadcasted_iota(I32, (tok, tok), 0) <= lax.broadcasted_iota(I32, (tok, tok), 1)
    rank = nn(jnp.broadcast_to(routed, (ROWS, tok)).astype(BF16), earlier.astype(BF16)) - 1.0
    row = lax.broadcasted_iota(I32, (ROWS, tok), 0)
    is_routed = jnp.broadcast_to(routed, (ROWS, tok)) > 0.5
    hit_in = is_routed & (rank == row.astype(F32))
    hit_gr = is_routed & (rank == (row - CAP).astype(F32))
    hit_in = jnp.where(hit_in & (row < CAP), 1.0, 0.0)
    hit_gr = jnp.where(hit_gr & (row >= CAP) & (row < 2 * CAP), 1.0, 0.0)
    slot_prob = jnp.sum(hit_gr * prob, axis=1, keepdims=True)
    hit_ref[...] = hit_in
    rows = nn(hit_in.astype(BF16), inp_ref[...]) + slot_prob * nn(hit_gr.astype(BF16), grad_ref[...])
    for d in range(n_dp):
        scratch[d] = rows[:, d * width : (d + 1) * width].astype(BF16)
    p = p_ref[0]
    for k in range(n_dp):
        outs[k][...] = scratch[p ^ k]


def slots(p, ids, prob, grad, inp, n_dp):
    tok, d_model = inp.shape
    width = d_model // n_dp
    return pl.pallas_call(
        slots_kernel,
        out_shape=[jax.ShapeDtypeStruct((ROWS, tok), F32)]
        + [jax.ShapeDtypeStruct((ROWS, width), BF16)] * n_dp,
        in_specs=[pl.BlockSpec(memory_space=SMEM)] + [pl.BlockSpec(memory_space=VMEM)] * 4,
        out_specs=[pl.BlockSpec(memory_space=VMEM)] * (n_dp + 1),
        scratch_shapes=[pltpu.VMEM((n_dp, ROWS, width), BF16)],
        name="slots",
    )(p, ids, prob, grad, inp)


def scale_kernel(factor_ref, w_ref, out_ref, *, tile):
    a = pl.program_id(0)
    r = pl.program_id(1)
    _, rows, cols = w_ref.shape
    for i in range(rows // tile):
        for j in range(cols // tile):
            at = (0, slice(i * tile, (i + 1) * tile), slice(j * tile, (j + 1) * tile))
            factor = factor_ref[a, r * (rows // tile) + i, j]
            out_ref[at] = (w_ref[at].astype(F32) * factor).astype(BF16)


def scale_weights(factor, w):
    import functools

    n, rows, cols = w.shape
    tile = rows // factor.shape[1]
    steps = 2 if factor.shape[1] % 2 == 0 else 1
    block = (1, rows // steps, cols)
    return pl.pallas_call(
        functools.partial(scale_kernel, tile=tile),
        grid=(n, steps),
        out_shape=jax.ShapeDtypeStruct(w.shape, BF16),
        in_specs=[
            pl.BlockSpec(memory_space=SMEM),
            pl.BlockSpec(block, lambda a, r: (a, r, 0)),
        ],
        out_specs=pl.BlockSpec(block, lambda a, r: (a, r, 0)),
        name="scale",
    )(factor, w)


def forward_kernel(p_ref, m0_ref, m1_ref, w_ref, x_ref, a_ref, b_ref, *, n_dp, n_z):
    slot_count = x_ref.shape[1]
    group = slot_count // n_dp
    span = m0_ref.shape[0]
    p = p_ref[0]
    col = lax.broadcasted_iota(I32, (1, span), 1)
    r = col & (ROWS - 1)
    pk = (col >> log2(ROWS)) & (n_dp - 1)
    zk = col >> (log2(ROWS) + log2(n_dp))
    line = lax.broadcasted_iota(I32, (slot_count, span), 0)

    def pick(low):
        total = None
        for ck, m_ref in enumerate((m0_ref, m1_ref)):
            slot = (p ^ pk) * group + (ck * n_z + zk) * CAP + (r - low)
            slot = jnp.where((r >= low) & (r < low + CAP), slot, -1)
            sel = jnp.where(line == slot, 1.0, 0.0).astype(BF16)
            part = nn(sel, m_ref[...])
            total = part if total is None else total + part
        return total.astype(BF16)

    x = pick(0)
    g = pick(CAP)
    x_ref[0] = x
    x_ref[1] = g
    half = a_ref.shape[2]
    for i, left in enumerate((x, x, g)):
        a_ref[i] = nn(left, w_ref[i, :, :half]).astype(BF16)
        b_ref[i] = nn(left, w_ref[i, :, half:]).astype(BF16)


def forward(p, m0, m1, w, n_dp, n_z):
    import functools

    slot_count = n_dp * CORES * n_z * CAP
    n, width, cols = w.shape
    part = jax.ShapeDtypeStruct((n, slot_count, cols // 2), BF16)
    return pl.pallas_call(
        functools.partial(forward_kernel, n_dp=n_dp, n_z=n_z),
        out_shape=[jax.ShapeDtypeStruct((2, slot_count, width), BF16), part, part],
        in_specs=[pl.BlockSpec(memory_space=SMEM)] + [pl.BlockSpec(memory_space=VMEM)] * 3,
        out_specs=[pl.BlockSpec(memory_space=VMEM)] * 3,
        name="forward",
    )(p, m0, m1, w)


def backward_kernel(p_ref, a_ref, ra_ref, b_ref, rb_ref, w_ref, g_ref, keep_ref, send_ref, *, n_dp, n_z):
    slot_count = g_ref.shape[1]
    group = slot_count // n_dp
    half = a_ref.shape[2]
    back = None
    for h, (u_ref, v_ref) in enumerate(((a_ref, ra_ref), (b_ref, rb_ref))):
        at = slice(h * half, (h + 1) * half)
        gate = u_ref[0].astype(F32) + v_ref[0].astype(F32)
        up = u_ref[1].astype(F32) + v_ref[1].astype(F32)
        down = u_ref[2].astype(F32) + v_ref[2].astype(F32)
        sig = jax.nn.sigmoid(gate)
        act = gate * sig
        gate_grad = (down * up * sig * (1.0 + gate * (1.0 - sig))).astype(BF16)
        up_grad = (down * act).astype(BF16)
        g_ref[0, :, at] = gate_grad
        g_ref[1, :, at] = up_grad
        g_ref[2, :, at] = (act * up).astype(BF16)
        part = nt(gate_grad, w_ref[0, :, at]) + nt(up_grad, w_ref[1, :, at])
        back = part if back is None else back + part
    back = back.astype(BF16)
    p = p_ref[0]
    rows = keep_ref.shape[0]
    capp = rows // (n_z * n_dp)
    for ck, out_ref in enumerate((keep_ref, send_ref)):
        o = lax.broadcasted_iota(I32, (rows, slot_count), 0)
        c = o & (capp - 1)
        pk = (o >> log2(capp)) & (n_dp - 1)
        zk = o >> (log2(capp) + log2(n_dp))
        slot = (p ^ pk) * group + (ck * n_z + zk) * CAP + c
        hit = (lax.broadcasted_iota(I32, (rows, slot_count), 1) == slot) & (c < CAP)
        out_ref[...] = nn(jnp.where(hit, 1.0, 0.0).astype(BF16), back).astype(BF16)


def backward(p, a, ra, b, rb, w, n_dp, n_z):
    import functools

    n, slot_count, half = a.shape
    width = w.shape[1]
    capp = 4
    out = jax.ShapeDtypeStruct((n_z * n_dp * capp, width), BF16)
    return pl.pallas_call(
        functools.partial(backward_kernel, n_dp=n_dp, n_z=n_z),
        out_shape=[jax.ShapeDtypeStruct((n, slot_count, 2 * half), BF16), out, out],
        in_specs=[pl.BlockSpec(memory_space=SMEM)] + [pl.BlockSpec(memory_space=VMEM)] * 5,
        out_specs=[pl.BlockSpec(memory_space=VMEM)] * 3,
        name="backward",
    )(p, a, ra, b, rb, w)


def weight_grad_kernel(x_ref, g_ref, out_ref):
    out_ref[0] = tn(x_ref[0], g_ref[0])


def weight_grad(x, g):
    n, slot_count, cols = g.shape
    width = x.shape[2]
    steps = 3 if width % (3 * 128) == 0 else 1
    tile = width // steps
    return pl.pallas_call(
        weight_grad_kernel,
        grid=(n, steps),
        out_shape=jax.ShapeDtypeStruct((n, width, cols), F32),
        in_specs=[
            pl.BlockSpec((1, slot_count, tile), lambda a, r: (a // 2, 0, r)),
            pl.BlockSpec((1, slot_count, cols), lambda a, r: (a, 0, 0)),
        ],
        out_specs=pl.BlockSpec((1, tile, cols), lambda a, r: (a, r, 0)),
        name="weight_grad",
    )(x, g)


def place_kernel(p_ref, hit_ref, *refs):
    parts, out_ref = refs[:-1], refs[-1]
    width = parts[0].shape[1]
    capp = parts[0].shape[0]
    p = p_ref[0]
    hit = hit_ref[:capp, :].astype(BF16)
    for k, part in enumerate(parts):
        at = pl.multiple_of((p ^ k) * width, 128)
        out_ref[:, pl.ds(at, width)] = tn(hit, part[...]).astype(BF16)


def place(p, hit, parts, tok):
    capp, width = parts[0].shape
    return pl.pallas_call(
        place_kernel,
        out_shape=jax.ShapeDtypeStruct((tok, width * len(parts)), BF16),
        in_specs=[pl.BlockSpec(memory_space=SMEM)]
        + [pl.BlockSpec(memory_space=VMEM)] * (1 + len(parts)),
        out_specs=pl.BlockSpec(memory_space=VMEM),
        name="place",
    )(p, hit, *parts)


def add_bf16(u, v):
    return (u.astype(F32) + v.astype(F32)).astype(BF16)


def per_device_fast(out_grad, layer_input, expert_ids, gate_prob, w_stack, scale_exps):
    n_dp = lax.axis_size("dp")
    n_ex = lax.axis_size("expert")
    n_z = n_ex // CORES
    tok = out_grad.shape[0]
    p = lax.axis_index("dp").astype(I32).reshape(1)
    hit, *blocks = slots(p, expert_ids.T, gate_prob.T, out_grad, layer_input, n_dp)
    factor = jnp.exp2(scale_exps.astype(F32))
    w = scale_weights(factor, w_stack)
    got = [blocks[0]] + [
        lax.ppermute(blocks[k], "dp", xor_pairs(n_dp, k)) for k in range(1, n_dp)
    ]
    mine = jnp.concatenate(got, axis=0)
    column = [mine] + [
        lax.ppermute(mine, "expert", xor_pairs(n_ex, k * CORES)) for k in range(1, n_z)
    ]
    m0 = jnp.concatenate(column, axis=0)
    m1 = lax.ppermute(m0, "expert", xor_pairs(n_ex, 1))
    x, a, b = forward(p, m0, m1, w, n_dp, n_z)
    ra = lax.ppermute(a, "dp", xor_pairs(n_dp, 1))
    rb = lax.ppermute(b, "dp", xor_pairs(n_dp, 2))
    a = add_bf16(a, ra)
    b = add_bf16(b, rb)
    ra = lax.ppermute(a, "dp", xor_pairs(n_dp, 2))
    rb = lax.ppermute(b, "dp", xor_pairs(n_dp, 1))
    g, keep, send = backward(p, a, ra, b, rb, w, n_dp, n_z)
    weight_grads = weight_grad(x, g)
    summed = add_bf16(keep, lax.ppermute(send, "expert", xor_pairs(n_ex, 1)))
    summed = summed.reshape(n_z, -1, summed.shape[1])
    total = summed[0].astype(F32)
    for k in range(1, n_z):
        total = total + lax.ppermute(summed[k], "expert", xor_pairs(n_ex, k * CORES)).astype(F32)
    total = total.astype(BF16).reshape(n_dp, -1, summed.shape[2])
    parts = [total[0]] + [
        lax.ppermute(total[k], "dp", xor_pairs(n_dp, k)) for k in range(1, n_dp)
    ]
    input_grad = place(p, hit, parts, tok)
    return input_grad, weight_grads


def per_device_any(out_grad, layer_input, expert_ids, gate_prob, w_stack, scale_exps):
    n_dp = lax.axis_size("dp")
    tok, d_model = out_grad.shape
    routed = expert_ids == 0
    mask = jnp.any(routed, axis=1)
    prob = jnp.sum(jnp.where(routed, gate_prob, 0.0), axis=1)
    rank = jnp.cumsum(mask.astype(I32)) - 1
    hit = ((rank[None, :] == jnp.arange(CAP)[:, None]) & mask[None, :]).astype(BF16)
    slot_input = jnp.dot(hit, layer_input, preferred_element_type=F32)
    slot_prob = jnp.sum(hit.astype(F32) * prob[None, :], axis=1)
    slot_grad = slot_prob[:, None] * jnp.dot(hit, out_grad, preferred_element_type=F32)
    both = jnp.stack([slot_input, slot_grad]).astype(BF16)
    both = both.reshape(2, CAP, n_dp, d_model // n_dp).transpose(2, 0, 1, 3)
    both = lax.all_to_all(both, "dp", split_axis=0, concat_axis=0, tiled=True)
    both = lax.all_gather(both, "expert", axis=0)
    both = both.transpose(2, 0, 1, 3, 4)
    lead = both.shape[1:4]
    both = both.reshape(2, -1, both.shape[-1])
    n, rows, cols = w_stack.shape
    factor = jnp.exp2(scale_exps.astype(F32))
    tiles = factor.shape[1:]
    w = w_stack.astype(F32).reshape(n, tiles[0], rows // tiles[0], tiles[1], cols // tiles[1])
    w = (w * factor[:, :, None, :, None]).reshape(n, rows, cols).astype(BF16)
    sides = jnp.stack([both[0], both[0], both[1]])
    partial = jnp.einsum("nrk,nkh->nrh", sides, w, preferred_element_type=F32)
    gate, up, down = lax.psum(partial, "dp")
    sig = jax.nn.sigmoid(gate)
    act = gate * sig
    gate_grad = (down * up * sig * (1.0 + gate * (1.0 - sig))).astype(BF16)
    up_grad = (down * act).astype(BF16)
    hidden = (act * up).astype(BF16)
    back = nt(gate_grad, w[0]) + nt(up_grad, w[1])
    back = lax.psum_scatter(back.reshape(lead + (rows,)), "expert", scatter_dimension=0, tiled=False)
    back = lax.all_to_all(back, "dp", split_axis=0, concat_axis=0, tiled=True)
    back = back.transpose(1, 0, 2).reshape(CAP, d_model)
    input_grad = tn(hit, back.astype(BF16)).astype(BF16)
    weight_grads = jnp.einsum(
        "nrd,nrh->ndh", sides, jnp.stack([gate_grad, up_grad, hidden]), preferred_element_type=F32
    )
    return input_grad, weight_grads


def solution(mesh):
    n_dp, n_ex = mesh.shape["dp"], mesh.shape["expert"]
    n_z = n_ex // CORES
    fast = n_dp == 4 and n_ex % CORES == 0 and is_pow2(n_z) and n_z <= 4
    in_specs = (
        P(("dp", "expert"), None),
        P(("dp", "expert"), None),
        P(("dp", "expert"), None),
        P(("dp", "expert"), None),
        P(None, "dp", "expert"),
        P(None, "dp", "expert"),
    )
    out_specs = (P(("dp", "expert"), None), P(None, "dp", "expert"))
    return jax.shard_map(
        per_device_fast if fast else per_device_any,
        mesh=mesh,
        in_specs=in_specs,
        out_specs=out_specs,
        check_vma=False,
    )
```

```python
import jax
import jax.numpy as jnp
from jax import lax
from jax.experimental import pallas as pl
from jax.experimental.pallas import tpu as pltpu
from jax.sharding import PartitionSpec as P

CAP = 3
BF16 = jnp.bfloat16
F32 = jnp.float32
I32 = jnp.int32
ROWS = 8
CHUNKS = 3
CORES = 2
LIMIT = 20 * 1024 * 1024
VMEM = pltpu.VMEM
SMEM = pltpu.SMEM


def in_hbm(x):
    return pltpu.with_memory_space_constraint(x, pltpu.HBM)


def log2(n):
    return n.bit_length() - 1


def is_pow2(n):
    return n & (n - 1) == 0


def xor_pairs(n, k):
    return [(i, i ^ k) for i in range(n)]


def nn(a, b):
    return lax.dot_general(a, b, (((1,), (0,)), ((), ())), preferred_element_type=F32)


def nt(a, b):
    return lax.dot_general(a, b, (((1,), (1,)), ((), ())), preferred_element_type=F32)


def tn(a, b):
    return lax.dot_general(a, b, (((0,), (0,)), ((), ())), preferred_element_type=F32)


def slots_kernel(p_ref, ids_hbm, prob_hbm, grad_hbm, inp_hbm, hit_ref, *refs):
    outs = refs[:-6]
    scratch, ids_ref, prob_ref, grad_ref, inp_ref, sem = refs[-6:]
    pairs = ((ids_hbm, ids_ref), (prob_hbm, prob_ref), (inp_hbm, inp_ref), (grad_hbm, grad_ref))
    copies = [pltpu.make_async_copy(u, v, sem.at[i]) for i, (u, v) in enumerate(pairs)]
    for copy in copies:
        copy.start()
    for copy in copies:
        copy.wait()
    n_dp = len(outs)
    width = outs[0].shape[1]
    tok = ids_ref.shape[1]
    named = ids_ref[...] == 0
    prob = jnp.sum(jnp.where(named, prob_ref[...], 0.0), axis=0, keepdims=True)
    routed = jnp.sum(named.astype(F32), axis=0, keepdims=True)
    earlier = lax.broadcasted_iota(I32, (tok, tok), 0) <= lax.broadcasted_iota(I32, (tok, tok), 1)
    rank = nn(jnp.broadcast_to(routed, (ROWS, tok)).astype(BF16), earlier.astype(BF16)) - 1.0
    row = lax.broadcasted_iota(I32, (ROWS, tok), 0)
    is_routed = jnp.broadcast_to(routed, (ROWS, tok)) > 0.5
    hit_in = is_routed & (rank == row.astype(F32))
    hit_gr = is_routed & (rank == (row - CAP).astype(F32))
    hit_in = jnp.where(hit_in & (row < CAP), 1.0, 0.0)
    hit_gr = jnp.where(hit_gr & (row >= CAP) & (row < 2 * CAP), 1.0, 0.0)
    slot_prob = jnp.sum(hit_gr * prob, axis=1, keepdims=True)
    hit_ref[...] = hit_in
    rows = nn(hit_in.astype(BF16), inp_ref[...]) + slot_prob * nn(hit_gr.astype(BF16), grad_ref[...])
    for d in range(n_dp):
        scratch[d] = rows[:, d * width : (d + 1) * width].astype(BF16)
    p = p_ref[0]
    for k in range(n_dp):
        outs[k][...] = scratch[p ^ k]


def slots(p, ids, prob, grad, inp, n_dp):
    tok, d_model = inp.shape
    width = d_model // n_dp
    return pl.pallas_call(
        slots_kernel,
        out_shape=[pltpu.VMEM((ROWS, tok), F32)] + [pltpu.VMEM((ROWS, width), BF16)] * n_dp,
        in_specs=[pl.BlockSpec(memory_space=SMEM)] + [pl.BlockSpec(memory_space=pltpu.HBM)] * 4,
        out_specs=[pl.BlockSpec(memory_space=VMEM)] * (n_dp + 1),
        scratch_shapes=[
            pltpu.VMEM((n_dp, ROWS, width), BF16),
            pltpu.VMEM(ids.shape, I32),
            pltpu.VMEM(prob.shape, F32),
            pltpu.VMEM(grad.shape, BF16),
            pltpu.VMEM(inp.shape, BF16),
            pltpu.SemaphoreType.DMA((4,)),
        ],
        compiler_params=pltpu.CompilerParams(vmem_limit_bytes=LIMIT),
        name="slots",
    )(p, *(in_hbm(v) for v in (ids, prob, grad, inp)))


def scale_kernel(factor_ref, w_ref, out_ref, sem):
    n, rows, cols = w_ref.shape
    tile = rows // factor_ref.shape[1]
    chunk = rows // CHUNKS if factor_ref.shape[1] % CHUNKS == 0 else rows
    copies = []
    for a in range(n):
        for c in range(rows // chunk):
            at = (a, pl.ds(c * chunk, chunk))
            copies.append(
                pltpu.make_async_copy(w_ref.at[at], out_ref.at[at], sem.at[len(copies)])
            )
    for copy in copies:
        copy.start()
    for step, copy in enumerate(copies):
        a, c = divmod(step, rows // chunk)
        copy.wait()
        for i in range(chunk // tile):
            for j in range(cols // tile):
                row = c * (chunk // tile) + i
                at = (a, slice(row * tile, (row + 1) * tile), slice(j * tile, (j + 1) * tile))
                out_ref[at] = out_ref[at] * factor_ref[a, row, j].astype(BF16)


def scale_weights(factor, w):
    n, rows, cols = w.shape
    return pl.pallas_call(
        scale_kernel,
        out_shape=pltpu.VMEM(w.shape, BF16),
        in_specs=[pl.BlockSpec(memory_space=SMEM), pl.BlockSpec(memory_space=pltpu.HBM)],
        out_specs=pl.BlockSpec(memory_space=VMEM),
        scratch_shapes=[pltpu.SemaphoreType.DMA((n * CHUNKS,))],
        compiler_params=pltpu.CompilerParams(vmem_limit_bytes=LIMIT),
        name="scale",
    )(factor, in_hbm(w))


def forward_kernel(p_ref, m0_ref, m1_ref, w_ref, x_ref, a_ref, b_ref, *, n_dp, n_z):
    slot_count = x_ref.shape[1]
    group = slot_count // n_dp
    span = m0_ref.shape[0]
    p = p_ref[0]
    col = lax.broadcasted_iota(I32, (1, span), 1)
    r = col & (ROWS - 1)
    pk = (col >> log2(ROWS)) & (n_dp - 1)
    zk = col >> (log2(ROWS) + log2(n_dp))
    line = lax.broadcasted_iota(I32, (slot_count, span), 0)

    def pick(low):
        total = None
        for ck, m_ref in enumerate((m0_ref, m1_ref)):
            slot = (p ^ pk) * group + (ck * n_z + zk) * CAP + (r - low)
            slot = jnp.where((r >= low) & (r < low + CAP), slot, -1)
            sel = jnp.where(line == slot, 1.0, 0.0).astype(BF16)
            part = nn(sel, m_ref[...])
            total = part if total is None else total + part
        return total.astype(BF16)

    x = pick(0)
    g = pick(CAP)
    x_ref[0] = x
    x_ref[1] = g
    half = a_ref.shape[2]
    for i, left in enumerate((x, x, g)):
        a_ref[i] = nn(left, w_ref[i, :, :half]).astype(BF16)
        b_ref[i] = nn(left, w_ref[i, :, half:]).astype(BF16)


def forward(p, m0, m1, w, n_dp, n_z):
    import functools

    slot_count = n_dp * CORES * n_z * CAP
    n, width, cols = w.shape
    part = jax.ShapeDtypeStruct((n, slot_count, cols // 2), BF16)
    return pl.pallas_call(
        functools.partial(forward_kernel, n_dp=n_dp, n_z=n_z),
        out_shape=[jax.ShapeDtypeStruct((2, slot_count, width), BF16), part, part],
        in_specs=[pl.BlockSpec(memory_space=SMEM)] + [pl.BlockSpec(memory_space=VMEM)] * 3,
        out_specs=[pl.BlockSpec(memory_space=VMEM)] * 3,
        compiler_params=pltpu.CompilerParams(vmem_limit_bytes=LIMIT),
        name="forward",
    )(p, m0, m1, w)


def backward_kernel(p_ref, a_ref, ra_ref, b_ref, rb_ref, w_ref, g_ref, keep_ref, send_ref, *, n_dp, n_z):
    slot_count = g_ref.shape[1]
    group = slot_count // n_dp
    half = a_ref.shape[2]
    back = None
    for h, (u_ref, v_ref) in enumerate(((a_ref, ra_ref), (b_ref, rb_ref))):
        at = slice(h * half, (h + 1) * half)
        gate = u_ref[0].astype(F32) + v_ref[0].astype(F32)
        up = u_ref[1].astype(F32) + v_ref[1].astype(F32)
        down = u_ref[2].astype(F32) + v_ref[2].astype(F32)
        sig = jax.nn.sigmoid(gate)
        act = gate * sig
        gate_grad = (down * up * sig * (1.0 + gate * (1.0 - sig))).astype(BF16)
        up_grad = (down * act).astype(BF16)
        g_ref[0, :, at] = gate_grad
        g_ref[1, :, at] = up_grad
        g_ref[2, :, at] = (act * up).astype(BF16)
        part = nt(gate_grad, w_ref[0, :, at]) + nt(up_grad, w_ref[1, :, at])
        back = part if back is None else back + part
    back = back.astype(BF16)
    p = p_ref[0]
    rows = keep_ref.shape[0]
    capp = rows // (n_z * n_dp)
    for ck, out_ref in enumerate((keep_ref, send_ref)):
        o = lax.broadcasted_iota(I32, (rows, slot_count), 0)
        c = o & (capp - 1)
        pk = (o >> log2(capp)) & (n_dp - 1)
        zk = o >> (log2(capp) + log2(n_dp))
        slot = (p ^ pk) * group + (ck * n_z + zk) * CAP + c
        hit = (lax.broadcasted_iota(I32, (rows, slot_count), 1) == slot) & (c < CAP)
        out_ref[...] = nn(jnp.where(hit, 1.0, 0.0).astype(BF16), back).astype(BF16)


def backward(p, a, ra, b, rb, w, n_dp, n_z):
    import functools

    n, slot_count, half = a.shape
    width = w.shape[1]
    capp = 4
    out = jax.ShapeDtypeStruct((n_z * n_dp * capp, width), BF16)
    return pl.pallas_call(
        functools.partial(backward_kernel, n_dp=n_dp, n_z=n_z),
        out_shape=[jax.ShapeDtypeStruct((n, slot_count, 2 * half), BF16), out, out],
        in_specs=[pl.BlockSpec(memory_space=SMEM)] + [pl.BlockSpec(memory_space=VMEM)] * 5,
        out_specs=[pl.BlockSpec(memory_space=VMEM)] * 3,
        compiler_params=pltpu.CompilerParams(vmem_limit_bytes=LIMIT),
        name="backward",
    )(p, a, ra, b, rb, w)


def weight_grad_kernel(x_ref, g_ref, out_ref):
    a = pl.program_id(0)
    tile = out_ref.shape[1]
    at = pl.multiple_of(pl.program_id(1) * tile, 128)
    out_ref[0] = tn(x_ref[a // 2, :, pl.ds(at, tile)], g_ref[a])


def weight_grad(x, g):
    n, slot_count, cols = g.shape
    width = x.shape[2]
    steps = 3 if width % (3 * 128) == 0 else 1
    tile = width // steps
    return pl.pallas_call(
        weight_grad_kernel,
        grid=(n, steps),
        out_shape=jax.ShapeDtypeStruct((n, width, cols), F32),
        in_specs=[pl.BlockSpec(memory_space=VMEM)] * 2,
        out_specs=pl.BlockSpec((1, tile, cols), lambda a, r: (a, r, 0)),
        compiler_params=pltpu.CompilerParams(vmem_limit_bytes=LIMIT),
        name="weight_grad",
    )(x, g)


def place_kernel(p_ref, hit_ref, *refs):
    parts, out_ref = refs[:-1], refs[-1]
    width = parts[0].shape[1]
    capp = parts[0].shape[0]
    p = p_ref[0]
    hit = hit_ref[:capp, :].astype(BF16)
    for k, part in enumerate(parts):
        at = pl.multiple_of((p ^ k) * width, 128)
        out_ref[:, pl.ds(at, width)] = tn(hit, part[...]).astype(BF16)


def place(p, hit, parts, tok):
    capp, width = parts[0].shape
    return pl.pallas_call(
        place_kernel,
        out_shape=jax.ShapeDtypeStruct((tok, width * len(parts)), BF16),
        in_specs=[pl.BlockSpec(memory_space=SMEM)]
        + [pl.BlockSpec(memory_space=VMEM)] * (1 + len(parts)),
        out_specs=pl.BlockSpec(memory_space=VMEM),
        compiler_params=pltpu.CompilerParams(vmem_limit_bytes=LIMIT),
        name="place",
    )(p, hit, *parts)


def add_bf16(u, v):
    return (u.astype(F32) + v.astype(F32)).astype(BF16)


def per_device_fast(out_grad, layer_input, expert_ids, gate_prob, w_stack, scale_exps):
    n_dp = lax.axis_size("dp")
    n_ex = lax.axis_size("expert")
    n_z = n_ex // CORES
    tok = out_grad.shape[0]
    p = lax.axis_index("dp").astype(I32).reshape(1)
    hit, *blocks = slots(p, expert_ids.T, gate_prob.T, out_grad, layer_input, n_dp)
    factor = jnp.exp2(scale_exps.astype(F32))
    w = scale_weights(factor, w_stack)
    got = [blocks[0]] + [
        lax.ppermute(blocks[k], "dp", xor_pairs(n_dp, k)) for k in range(1, n_dp)
    ]
    mine = jnp.concatenate(got, axis=0)
    column = [mine] + [
        lax.ppermute(mine, "expert", xor_pairs(n_ex, k * CORES)) for k in range(1, n_z)
    ]
    m0 = jnp.concatenate(column, axis=0)
    m1 = lax.ppermute(m0, "expert", xor_pairs(n_ex, 1))
    x, a, b = forward(p, m0, m1, w, n_dp, n_z)
    ra = lax.ppermute(a, "dp", xor_pairs(n_dp, 1))
    rb = lax.ppermute(b, "dp", xor_pairs(n_dp, 2))
    a = add_bf16(a, ra)
    b = add_bf16(b, rb)
    ra = lax.ppermute(a, "dp", xor_pairs(n_dp, 2))
    rb = lax.ppermute(b, "dp", xor_pairs(n_dp, 1))
    g, keep, send = backward(p, a, ra, b, rb, w, n_dp, n_z)
    weight_grads = weight_grad(x, g)
    summed = add_bf16(keep, lax.ppermute(send, "expert", xor_pairs(n_ex, 1)))
    summed = summed.reshape(n_z, -1, summed.shape[1])
    total = summed[0].astype(F32)
    for k in range(1, n_z):
        total = total + lax.ppermute(summed[k], "expert", xor_pairs(n_ex, k * CORES)).astype(F32)
    total = total.astype(BF16).reshape(n_dp, -1, summed.shape[2])
    parts = [total[0]] + [
        lax.ppermute(total[k], "dp", xor_pairs(n_dp, k)) for k in range(1, n_dp)
    ]
    input_grad = place(p, hit, parts, tok)
    return input_grad, weight_grads


def per_device_any(out_grad, layer_input, expert_ids, gate_prob, w_stack, scale_exps):
    n_dp = lax.axis_size("dp")
    tok, d_model = out_grad.shape
    routed = expert_ids == 0
    mask = jnp.any(routed, axis=1)
    prob = jnp.sum(jnp.where(routed, gate_prob, 0.0), axis=1)
    rank = jnp.cumsum(mask.astype(I32)) - 1
    hit = ((rank[None, :] == jnp.arange(CAP)[:, None]) & mask[None, :]).astype(BF16)
    slot_input = jnp.dot(hit, layer_input, preferred_element_type=F32)
    slot_prob = jnp.sum(hit.astype(F32) * prob[None, :], axis=1)
    slot_grad = slot_prob[:, None] * jnp.dot(hit, out_grad, preferred_element_type=F32)
    both = jnp.stack([slot_input, slot_grad]).astype(BF16)
    both = both.reshape(2, CAP, n_dp, d_model // n_dp).transpose(2, 0, 1, 3)
    both = lax.all_to_all(both, "dp", split_axis=0, concat_axis=0, tiled=True)
    both = lax.all_gather(both, "expert", axis=0)
    both = both.transpose(2, 0, 1, 3, 4)
    lead = both.shape[1:4]
    both = both.reshape(2, -1, both.shape[-1])
    n, rows, cols = w_stack.shape
    factor = jnp.exp2(scale_exps.astype(F32))
    tiles = factor.shape[1:]
    w = w_stack.astype(F32).reshape(n, tiles[0], rows // tiles[0], tiles[1], cols // tiles[1])
    w = (w * factor[:, :, None, :, None]).reshape(n, rows, cols).astype(BF16)
    sides = jnp.stack([both[0], both[0], both[1]])
    partial = jnp.einsum("nrk,nkh->nrh", sides, w, preferred_element_type=F32)
    gate, up, down = lax.psum(partial, "dp")
    sig = jax.nn.sigmoid(gate)
    act = gate * sig
    gate_grad = (down * up * sig * (1.0 + gate * (1.0 - sig))).astype(BF16)
    up_grad = (down * act).astype(BF16)
    hidden = (act * up).astype(BF16)
    back = nt(gate_grad, w[0]) + nt(up_grad, w[1])
    back = lax.psum_scatter(back.reshape(lead + (rows,)), "expert", scatter_dimension=0, tiled=False)
    back = lax.all_to_all(back, "dp", split_axis=0, concat_axis=0, tiled=True)
    back = back.transpose(1, 0, 2).reshape(CAP, d_model)
    input_grad = tn(hit, back.astype(BF16)).astype(BF16)
    weight_grads = jnp.einsum(
        "nrd,nrh->ndh", sides, jnp.stack([gate_grad, up_grad, hidden]), preferred_element_type=F32
    )
    return input_grad, weight_grads


def solution(mesh):
    n_dp, n_ex = mesh.shape["dp"], mesh.shape["expert"]
    n_z = n_ex // CORES
    fast = n_dp == 4 and n_ex % CORES == 0 and is_pow2(n_z) and n_z <= 4
    in_specs = (
        P(("dp", "expert"), None),
        P(("dp", "expert"), None),
        P(("dp", "expert"), None),
        P(("dp", "expert"), None),
        P(None, "dp", "expert"),
        P(None, "dp", "expert"),
    )
    out_specs = (P(("dp", "expert"), None), P(None, "dp", "expert"))
    return jax.shard_map(
        per_device_fast if fast else per_device_any,
        mesh=mesh,
        in_specs=in_specs,
        out_specs=out_specs,
        check_vma=False,
    )
```

```python
import functools

import jax
import jax.numpy as jnp
from jax import lax
from jax.experimental import pallas as pl
from jax.experimental.pallas import tpu as pltpu
from jax.sharding import PartitionSpec as P


CAP = 3
BF16 = jnp.bfloat16
F32 = jnp.float32
I32 = jnp.int32
ROWS = 8
CHUNKS = 3
CAPP = 4
CORES = 2
LIMIT = 20 * 1024 * 1024
VMEM = pltpu.VMEM
SMEM = pltpu.SMEM


def in_hbm(x):
    return pltpu.with_memory_space_constraint(x, pltpu.HBM)


def log2(n):
    return n.bit_length() - 1


def is_pow2(n):
    return n & (n - 1) == 0


def xor_pairs(n, k):
    return [(i, i ^ k) for i in range(n)]


def nn(a, b):
    return lax.dot_general(a, b, (((1,), (0,)), ((), ())), preferred_element_type=F32)


def nt(a, b):
    return lax.dot_general(a, b, (((1,), (1,)), ((), ())), preferred_element_type=F32)


def tn(a, b):
    return lax.dot_general(a, b, (((0,), (0,)), ((), ())), preferred_element_type=F32)


def slots_kernel(p_ref, ids_hbm, prob_hbm, grad_hbm, inp_hbm, hit_ref, *refs):
    outs = refs[:-6]
    scratch, ids_ref, prob_ref, grad_ref, inp_ref, sem = refs[-6:]
    pairs = ((ids_hbm, ids_ref), (prob_hbm, prob_ref), (inp_hbm, inp_ref), (grad_hbm, grad_ref))
    copies = [pltpu.make_async_copy(u, v, sem.at[i]) for i, (u, v) in enumerate(pairs)]
    for copy in copies:
        copy.start()
    for copy in copies:
        copy.wait()
    n_dp = len(outs)
    width = outs[0].shape[1]
    tok = ids_ref.shape[1]
    named = ids_ref[...] == 0
    prob = jnp.sum(jnp.where(named, prob_ref[...], 0.0), axis=0, keepdims=True)
    routed = jnp.sum(named.astype(F32), axis=0, keepdims=True)
    earlier = lax.broadcasted_iota(I32, (tok, tok), 0) <= lax.broadcasted_iota(I32, (tok, tok), 1)
    rank = nn(jnp.broadcast_to(routed, (ROWS, tok)).astype(BF16), earlier.astype(BF16)) - 1.0
    row = lax.broadcasted_iota(I32, (ROWS, tok), 0)
    is_routed = jnp.broadcast_to(routed, (ROWS, tok)) > 0.5
    hit_in = is_routed & (rank == row.astype(F32))
    hit_gr = is_routed & (rank == (row - CAP).astype(F32))
    hit_in = jnp.where(hit_in & (row < CAP), 1.0, 0.0)
    hit_gr = jnp.where(hit_gr & (row >= CAP) & (row < 2 * CAP), 1.0, 0.0)
    slot_prob = jnp.sum(hit_gr * prob, axis=1, keepdims=True)
    hit_ref[...] = hit_in
    rows = nn(hit_in.astype(BF16), inp_ref[...]) + slot_prob * nn(hit_gr.astype(BF16), grad_ref[...])
    for d in range(n_dp):
        scratch[d] = rows[:, d * width : (d + 1) * width].astype(BF16)
    p = p_ref[0]
    for k in range(n_dp):
        outs[k][...] = scratch[p ^ k]


def slots(p, ids, prob, grad, inp, n_dp):
    tok, d_model = inp.shape
    width = d_model // n_dp
    return pl.pallas_call(
        slots_kernel,
        out_shape=[pltpu.VMEM((ROWS, tok), F32)] + [pltpu.VMEM((ROWS, width), BF16)] * n_dp,
        in_specs=[pl.BlockSpec(memory_space=SMEM)] + [pl.BlockSpec(memory_space=pltpu.HBM)] * 4,
        out_specs=[pl.BlockSpec(memory_space=VMEM)] * (n_dp + 1),
        scratch_shapes=[
            pltpu.VMEM((n_dp, ROWS, width), BF16),
            pltpu.VMEM(ids.shape, I32),
            pltpu.VMEM(prob.shape, F32),
            pltpu.VMEM(grad.shape, BF16),
            pltpu.VMEM(inp.shape, BF16),
            pltpu.SemaphoreType.DMA((4,)),
        ],
        compiler_params=pltpu.CompilerParams(vmem_limit_bytes=LIMIT),
        name="slots",
    )(p, *(in_hbm(v) for v in (ids, prob, grad, inp)))


def scale_kernel(exp_hbm, w_ref, out_ref, exp_ref, sem):
    exp_copy = pltpu.make_async_copy(exp_hbm, exp_ref, sem.at[sem.shape[0] - 1])
    exp_copy.start()
    n, rows, cols = w_ref.shape
    tile = rows // exp_ref.shape[1]
    chunk = rows // CHUNKS if exp_ref.shape[1] % CHUNKS == 0 else rows
    copies = []
    for a in range(n):
        for c in range(rows // chunk):
            at = (a, pl.ds(c * chunk, chunk))
            copies.append(
                pltpu.make_async_copy(w_ref.at[at], out_ref.at[at], sem.at[len(copies)])
            )
    for copy in copies:
        copy.start()
    exp_copy.wait()
    for step, copy in enumerate(copies):
        a, c = divmod(step, rows // chunk)
        copy.wait()
        for i in range(chunk // tile):
            for j in range(cols // tile):
                row = c * (chunk // tile) + i
                at = (a, slice(row * tile, (row + 1) * tile), slice(j * tile, (j + 1) * tile))
                e = exp_ref[a, row, j]
                factor = jnp.where(e > 0, 2.0, jnp.where(e < 0, 0.5, 1.0))
                out_ref[at] = out_ref[at] * factor.astype(BF16)


def scale_weights(exps, w):
    n, _, _ = w.shape
    return pl.pallas_call(
        scale_kernel,
        out_shape=pltpu.VMEM(w.shape, BF16),
        in_specs=[pl.BlockSpec(memory_space=pltpu.HBM)] * 2,
        out_specs=pl.BlockSpec(memory_space=VMEM),
        scratch_shapes=[
            pltpu.SMEM(exps.shape, I32),
            pltpu.SemaphoreType.DMA((n * CHUNKS + 1,)),
        ],
        compiler_params=pltpu.CompilerParams(vmem_limit_bytes=LIMIT),
        name="scale",
    )(in_hbm(exps), in_hbm(w))


def forward_kernel(p_ref, m_ref, w_ref, x_ref, a_ref, b_ref, *, n_dp):
    slot_count = x_ref.shape[1]
    group = slot_count // n_dp
    span = m_ref.shape[0]
    p = p_ref[0]
    col = lax.broadcasted_iota(I32, (1, span), 1)
    r = col & (ROWS - 1)
    pk = (col >> log2(ROWS)) & (n_dp - 1)
    zk = col >> (log2(ROWS) + log2(n_dp))
    line = lax.broadcasted_iota(I32, (slot_count, span), 0)

    def pick(low):
        slot = (p ^ pk) * group + zk * CAP + (r - low)
        slot = jnp.where((r >= low) & (r < low + CAP), slot, -1)
        sel = jnp.where(line == slot, 1.0, 0.0).astype(BF16)
        return nn(sel, m_ref[...]).astype(BF16)

    x = pick(0)
    g = pick(CAP)
    x_ref[0] = x
    x_ref[1] = g
    half = a_ref.shape[2]
    for i, left in enumerate((x, x, g)):
        a_ref[i] = nn(left, w_ref[i, :, :half]).astype(BF16)
        b_ref[i] = nn(left, w_ref[i, :, half:]).astype(BF16)


def forward(p, m, w, n_dp, n_z):
    slot_count = n_dp * n_z * CAP
    n, width, cols = w.shape
    part = pltpu.VMEM((n, slot_count, cols // 2), BF16)
    return pl.pallas_call(
        functools.partial(forward_kernel, n_dp=n_dp),
        out_shape=[pltpu.VMEM((2, slot_count, width), BF16), part, part],
        in_specs=[pl.BlockSpec(memory_space=SMEM)] + [pl.BlockSpec(memory_space=VMEM)] * 2,
        out_specs=[pl.BlockSpec(memory_space=VMEM)] * 3,
        compiler_params=pltpu.CompilerParams(vmem_limit_bytes=LIMIT),
        name="forward",
    )(p, m, w)


def backward_kernel(p_ref, a_ref, ra_ref, b_ref, rb_ref, w_ref, g_ref, out_ref, *, n_dp, n_z):
    slot_count = g_ref.shape[1]
    group = slot_count // n_dp
    half = a_ref.shape[2]
    back = None
    for h, (u_ref, v_ref) in enumerate(((a_ref, ra_ref), (b_ref, rb_ref))):
        at = slice(h * half, (h + 1) * half)
        gate = u_ref[0].astype(F32) + v_ref[0].astype(F32)
        up = u_ref[1].astype(F32) + v_ref[1].astype(F32)
        down = u_ref[2].astype(F32) + v_ref[2].astype(F32)
        sig = jax.nn.sigmoid(gate)
        act = gate * sig
        gate_grad = (down * up * sig * (1.0 + gate * (1.0 - sig))).astype(BF16)
        up_grad = (down * act).astype(BF16)
        g_ref[0, :, at] = gate_grad
        g_ref[1, :, at] = up_grad
        g_ref[2, :, at] = (act * up).astype(BF16)
        part = nt(gate_grad, w_ref[0, :, at]) + nt(up_grad, w_ref[1, :, at])
        back = part if back is None else back + part
    back = back.astype(BF16)
    p = p_ref[0]
    rows = out_ref.shape[0]
    capp = rows // (n_z * n_dp)
    o = lax.broadcasted_iota(I32, (rows, slot_count), 0)
    c = o & (capp - 1)
    pk = (o >> log2(capp)) & (n_dp - 1)
    zk = o >> (log2(capp) + log2(n_dp))
    slot = (p ^ pk) * group + zk * CAP + c
    hit = (lax.broadcasted_iota(I32, (rows, slot_count), 1) == slot) & (c < CAP)
    out_ref[...] = nn(jnp.where(hit, 1.0, 0.0).astype(BF16), back).astype(BF16)


def backward(p, a, ra, b, rb, w, n_dp, n_z):
    n, slot_count, half = a.shape
    width = w.shape[1]
    return pl.pallas_call(
        functools.partial(backward_kernel, n_dp=n_dp, n_z=n_z),
        out_shape=[
            pltpu.VMEM((n, slot_count, 2 * half), BF16),
            pltpu.VMEM((n_z * n_dp * CAPP, width), BF16),
        ],
        in_specs=[pl.BlockSpec(memory_space=SMEM)] + [pl.BlockSpec(memory_space=VMEM)] * 5,
        out_specs=[pl.BlockSpec(memory_space=VMEM)] * 2,
        compiler_params=pltpu.CompilerParams(vmem_limit_bytes=LIMIT),
        name="backward",
    )(p, a, ra, b, rb, w)


def weight_grad_kernel(*refs, planes, tile):
    x0_ref, x1_ref, g0_ref, g1_ref = refs[:4]
    out_ref, scratch, sem = refs[-3:]
    width = x0_ref.shape[2]
    copies = []
    for a in planes:
        x = jnp.concatenate([x0_ref[a // 2], x1_ref[a // 2]], axis=0)
        g = jnp.concatenate([g0_ref[a], g1_ref[a]], axis=0)
        for r in range(0, width, tile):
            i = len(copies)
            scratch[i] = tn(x[:, r : r + tile], g)
            copy = pltpu.make_async_copy(scratch.at[i], out_ref.at[a, pl.ds(r, tile)], sem.at[i])
            copy.start()
            copies.append(copy)
    for copy in copies:
        copy.wait()


def weight_grad(planes, x0, x1, g0, g1, total=None):
    n, _, cols = g0.shape
    width = x0.shape[2]
    tile = width // 3 if width % (3 * 128) == 0 else width
    steps = len(planes) * (width // tile)
    operands = [x0, x1, g0, g1] + ([] if total is None else [total])
    return pl.pallas_call(
        functools.partial(weight_grad_kernel, planes=planes, tile=tile),
        out_shape=pltpu.HBM((n, width, cols), F32),
        in_specs=[pl.BlockSpec(memory_space=VMEM)] * 4
        + [pl.BlockSpec(memory_space=pltpu.HBM)] * (len(operands) - 4),
        out_specs=pl.BlockSpec(memory_space=pltpu.HBM),
        scratch_shapes=[
            pltpu.VMEM((steps, tile, cols), F32),
            pltpu.SemaphoreType.DMA((steps,)),
        ],
        input_output_aliases={} if total is None else {4: 0},
        compiler_params=pltpu.CompilerParams(vmem_limit_bytes=LIMIT),
        name="weight_grad",
    )(*operands)


def place_kernel(p_ref, hit_ref, *refs):
    parts, out_ref = refs[:-1], refs[-1]
    width = parts[0].shape[1]
    capp = parts[0].shape[0]
    p = p_ref[0]
    hit = hit_ref[:capp, :].astype(BF16)
    for k, part in enumerate(parts):
        at = pl.multiple_of((p ^ k) * width, 128)
        out_ref[:, pl.ds(at, width)] = tn(hit, part[...]).astype(BF16)


def place(p, hit, parts, tok):
    _, width = parts[0].shape
    return pl.pallas_call(
        place_kernel,
        out_shape=jax.ShapeDtypeStruct((tok, width * len(parts)), BF16),
        in_specs=[pl.BlockSpec(memory_space=SMEM)]
        + [pl.BlockSpec(memory_space=VMEM)] * (1 + len(parts)),
        out_specs=pl.BlockSpec(memory_space=VMEM),
        compiler_params=pltpu.CompilerParams(vmem_limit_bytes=LIMIT),
        name="place",
    )(p, hit, *parts)


def add_bf16(u, v):
    return (u.astype(F32) + v.astype(F32)).astype(BF16)


def shift(x, axis, k):
    return lax.ppermute(x, axis, xor_pairs(lax.axis_size(axis), k))


def per_device_fast(out_grad, layer_input, expert_ids, gate_prob, w_stack, scale_exps):
    return fast_body(out_grad, layer_input, expert_ids, gate_prob, w_stack, scale_exps)


def fast_body(out_grad, layer_input, expert_ids, gate_prob, w_stack, scale_exps):
    n_dp = lax.axis_size("dp")
    n_z = lax.axis_size("expert") // CORES
    tok = out_grad.shape[0]
    p = lax.axis_index("dp").astype(I32).reshape(1)
    hit, *blocks = slots(p, expert_ids.T, gate_prob.T, out_grad, layer_input, n_dp)
    w = scale_weights(scale_exps, w_stack)
    got = [blocks[0]] + [shift(blocks[k], "dp", k) for k in range(1, n_dp)]
    mine = jnp.concatenate(got, axis=0)
    column = [mine] + [shift(mine, "expert", k * CORES) for k in range(1, n_z)]
    m0 = jnp.concatenate(column, axis=0)
    m1 = shift(m0, "expert", 1)
    xs, sums = [], []
    for m in (m0, m1):
        x, a, b = forward(p, m, w, n_dp, n_z)
        ra = shift(a, "dp", 1)
        rb = shift(b, "dp", 2)
        a = add_bf16(a, ra)
        b = add_bf16(b, rb)
        ra = shift(a, "dp", 2)
        rb = shift(b, "dp", 1)
        xs.append(x)
        sums.append((a, ra, b, rb))
    gs, outs = [], []
    for a, ra, b, rb in sums:
        g, out = backward(p, a, ra, b, rb, w, n_dp, n_z)
        gs.append(g)
        outs.append(out)
    weight_grads = weight_grad((0,), *xs, *gs)
    weight_grads = weight_grad((1, 2), *xs, *gs, weight_grads)
    summed = add_bf16(outs[0], shift(outs[1], "expert", 1))
    summed = summed.reshape(n_z, -1, summed.shape[1])
    total = summed[0].astype(F32)
    for k in range(1, n_z):
        total = total + shift(summed[k], "expert", k * CORES).astype(F32)
    total = total.astype(BF16).reshape(n_dp, -1, summed.shape[2])
    parts = [total[0]] + [shift(total[k], "dp", k) for k in range(1, n_dp)]
    input_grad = place(p, hit, parts, tok)
    return input_grad, weight_grads


def per_device_any(out_grad, layer_input, expert_ids, gate_prob, w_stack, scale_exps):
    n_dp = lax.axis_size("dp")
    _, d_model = out_grad.shape
    routed = expert_ids == 0
    mask = jnp.any(routed, axis=1)
    prob = jnp.sum(jnp.where(routed, gate_prob, 0.0), axis=1)
    rank = jnp.cumsum(mask.astype(I32)) - 1
    hit = ((rank[None, :] == jnp.arange(CAP)[:, None]) & mask[None, :]).astype(BF16)
    slot_input = jnp.dot(hit, layer_input, preferred_element_type=F32)
    slot_prob = jnp.sum(hit.astype(F32) * prob[None, :], axis=1)
    slot_grad = slot_prob[:, None] * jnp.dot(hit, out_grad, preferred_element_type=F32)
    both = jnp.stack([slot_input, slot_grad]).astype(BF16)
    both = both.reshape(2, CAP, n_dp, d_model // n_dp).transpose(2, 0, 1, 3)
    both = lax.all_to_all(both, "dp", split_axis=0, concat_axis=0, tiled=True)
    both = lax.all_gather(both, "expert", axis=0)
    both = both.transpose(2, 0, 1, 3, 4)
    lead = both.shape[1:4]
    both = both.reshape(2, -1, both.shape[-1])
    n, rows, cols = w_stack.shape
    factor = jnp.exp2(scale_exps.astype(F32))
    tiles = factor.shape[1:]
    w = w_stack.astype(F32).reshape(n, tiles[0], rows // tiles[0], tiles[1], cols // tiles[1])
    w = (w * factor[:, :, None, :, None]).reshape(n, rows, cols).astype(BF16)
    sides = jnp.stack([both[0], both[0], both[1]])
    partial = jnp.einsum("nrk,nkh->nrh", sides, w, preferred_element_type=F32)
    gate, up, down = lax.psum(partial, "dp")
    sig = jax.nn.sigmoid(gate)
    act = gate * sig
    gate_grad = (down * up * sig * (1.0 + gate * (1.0 - sig))).astype(BF16)
    up_grad = (down * act).astype(BF16)
    hidden = (act * up).astype(BF16)
    back = nt(gate_grad, w[0]) + nt(up_grad, w[1])
    back = lax.psum_scatter(back.reshape(lead + (rows,)), "expert", scatter_dimension=0, tiled=False)
    back = lax.all_to_all(back, "dp", split_axis=0, concat_axis=0, tiled=True)
    back = back.transpose(1, 0, 2).reshape(CAP, d_model)
    input_grad = tn(hit, back.astype(BF16)).astype(BF16)
    weight_grads = jnp.einsum(
        "nrd,nrh->ndh", sides, jnp.stack([gate_grad, up_grad, hidden]), preferred_element_type=F32
    )
    return input_grad, weight_grads


def solution(mesh):
    n_dp, n_ex = mesh.shape["dp"], mesh.shape["expert"]
    n_z = n_ex // CORES
    fast = n_dp == 4 and n_ex % CORES == 0 and is_pow2(n_z) and n_z <= 4
    in_specs = (
        P(("dp", "expert"), None),
        P(("dp", "expert"), None),
        P(("dp", "expert"), None),
        P(("dp", "expert"), None),
        P(None, "dp", "expert"),
        P(None, "dp", "expert"),
    )
    out_specs = (P(("dp", "expert"), None), P(None, "dp", "expert"))
    return jax.shard_map(
        per_device_fast if fast else per_device_any,
        mesh=mesh,
        in_specs=in_specs,
        out_specs=out_specs,
        check_vma=False,
    )
```

```python
import functools

import jax
import jax.numpy as jnp
from jax import lax
from jax.experimental import pallas as pl
from jax.experimental.pallas import tpu as pltpu
from jax.sharding import PartitionSpec as P


CAP = 3
BF16 = jnp.bfloat16
F32 = jnp.float32
I32 = jnp.int32
ROWS = 8
CHUNKS = 3
CAPP = 4
CORES = 2
LIMIT = 20 * 1024 * 1024
VMEM = pltpu.VMEM
SMEM = pltpu.SMEM


def in_hbm(x):
    return pltpu.with_memory_space_constraint(x, pltpu.HBM)


def log2(n):
    return n.bit_length() - 1


def is_pow2(n):
    return n & (n - 1) == 0


def xor_pairs(n, k):
    return [(i, i ^ k) for i in range(n)]


def nn(a, b):
    return lax.dot_general(a, b, (((1,), (0,)), ((), ())), preferred_element_type=F32)


def nt(a, b):
    return lax.dot_general(a, b, (((1,), (1,)), ((), ())), preferred_element_type=F32)


def tn(a, b):
    return lax.dot_general(a, b, (((0,), (0,)), ((), ())), preferred_element_type=F32)


def slots_kernel(p_ref, e_ref, ids_hbm, prob_hbm, grad_hbm, inp_hbm, hit_ref, *refs):
    outs = refs[:-6]
    scratch, ids_ref, prob_ref, grad_ref, inp_ref, sem = refs[-6:]
    pairs = ((ids_hbm, ids_ref), (prob_hbm, prob_ref), (inp_hbm, inp_ref), (grad_hbm, grad_ref))
    copies = [pltpu.make_async_copy(u, v, sem.at[i]) for i, (u, v) in enumerate(pairs)]
    for copy in copies:
        copy.start()
    for copy in copies:
        copy.wait()
    n_dp = len(outs)
    width = outs[0].shape[1]
    tok = ids_ref.shape[1]
    named = ids_ref[...] == 0
    prob = jnp.sum(jnp.where(named, prob_ref[...], 0.0), axis=0, keepdims=True)
    routed = jnp.sum(named.astype(F32), axis=0, keepdims=True)
    earlier = lax.broadcasted_iota(I32, (tok, tok), 0) <= lax.broadcasted_iota(I32, (tok, tok), 1)
    rank = nn(jnp.broadcast_to(routed, (ROWS, tok)).astype(BF16), earlier.astype(BF16)) - 1.0
    row = lax.broadcasted_iota(I32, (ROWS, tok), 0)
    is_routed = jnp.broadcast_to(routed, (ROWS, tok)) > 0.5
    hit_in = is_routed & (rank == row.astype(F32))
    hit_gr = is_routed & (rank == (row - CAP).astype(F32))
    hit_in = jnp.where(hit_in & (row < CAP), 1.0, 0.0)
    hit_gr = jnp.where(hit_gr & (row >= CAP) & (row < 2 * CAP), 1.0, 0.0)
    slot_prob = jnp.sum(hit_gr * prob, axis=1, keepdims=True)
    hit_ref[...] = hit_in
    rows = nn(hit_in.astype(BF16), inp_ref[...]) + slot_prob * nn(hit_gr.astype(BF16), grad_ref[...])
    for d in range(n_dp):
        scratch[d] = rows[:, d * width : (d + 1) * width].astype(BF16)
    p = p_ref[0]
    for k in range(n_dp):
        outs[k][...] = scratch[p ^ k]


def slots(p, e, ids, prob, grad, inp, n_dp):
    tok, d_model = inp.shape
    width = d_model // n_dp
    return pl.pallas_call(
        slots_kernel,
        out_shape=[pltpu.VMEM((ROWS, tok), F32)] + [pltpu.VMEM((ROWS, width), BF16)] * n_dp,
        in_specs=[pl.BlockSpec(memory_space=SMEM)] * 2 + [pl.BlockSpec(memory_space=pltpu.HBM)] * 4,
        out_specs=[pl.BlockSpec(memory_space=VMEM)] * (n_dp + 1),
        scratch_shapes=[
            pltpu.VMEM((n_dp, ROWS, width), BF16),
            pltpu.VMEM(ids.shape, I32),
            pltpu.VMEM(prob.shape, F32),
            pltpu.VMEM(grad.shape, BF16),
            pltpu.VMEM(inp.shape, BF16),
            pltpu.SemaphoreType.DMA((4,)),
        ],
        compiler_params=pltpu.CompilerParams(vmem_limit_bytes=LIMIT),
        name="slots",
    )(p, e, *(in_hbm(v) for v in (ids, prob, grad, inp)))


def scale_kernel(exp_hbm, w_ref, out_ref, exp_ref, sem):
    exp_copy = pltpu.make_async_copy(exp_hbm, exp_ref, sem.at[sem.shape[0] - 1])
    exp_copy.start()
    n, rows, cols = w_ref.shape
    tile = rows // exp_ref.shape[1]
    chunk = rows // CHUNKS if exp_ref.shape[1] % CHUNKS == 0 else rows
    copies = []
    for a in range(n):
        for c in range(rows // chunk):
            at = (a, pl.ds(c * chunk, chunk))
            copies.append(
                pltpu.make_async_copy(w_ref.at[at], out_ref.at[at], sem.at[len(copies)])
            )
    for copy in copies:
        copy.start()
    exp_copy.wait()
    for step, copy in enumerate(copies):
        a, c = divmod(step, rows // chunk)
        copy.wait()
        for i in range(chunk // tile):
            for j in range(cols // tile):
                row = c * (chunk // tile) + i
                at = (a, slice(row * tile, (row + 1) * tile), slice(j * tile, (j + 1) * tile))
                e = exp_ref[a, row, j]
                factor = jnp.where(e > 0, 2.0, jnp.where(e < 0, 0.5, 1.0))
                out_ref[at] = out_ref[at] * factor.astype(BF16)


def scale_weights(exps, w):
    n, _, _ = w.shape
    return pl.pallas_call(
        scale_kernel,
        out_shape=pltpu.VMEM(w.shape, BF16),
        in_specs=[pl.BlockSpec(memory_space=pltpu.HBM)] * 2,
        out_specs=pl.BlockSpec(memory_space=VMEM),
        scratch_shapes=[
            pltpu.SMEM(exps.shape, I32),
            pltpu.SemaphoreType.DMA((n * CHUNKS + 1,)),
        ],
        compiler_params=pltpu.CompilerParams(vmem_limit_bytes=LIMIT),
        name="scale",
    )(in_hbm(exps), in_hbm(w))


def forward_kernel(p_ref, m_ref, w_ref, x_ref, a_ref, b_ref, *, n_dp):
    slot_count = x_ref.shape[1]
    group = slot_count // n_dp
    span = m_ref.shape[0]
    p = p_ref[0]
    col = lax.broadcasted_iota(I32, (1, span), 1)
    r = col & (ROWS - 1)
    pk = (col >> log2(ROWS)) & (n_dp - 1)
    zk = col >> (log2(ROWS) + log2(n_dp))
    line = lax.broadcasted_iota(I32, (slot_count, span), 0)

    def pick(low):
        slot = (p ^ pk) * group + zk * CAP + (r - low)
        slot = jnp.where((r >= low) & (r < low + CAP), slot, -1)
        sel = jnp.where(line == slot, 1.0, 0.0).astype(BF16)
        return nn(sel, m_ref[...]).astype(BF16)

    x = pick(0)
    g = pick(CAP)
    x_ref[0] = x
    x_ref[1] = g
    half = a_ref.shape[2]
    for i, left in enumerate((x, x, g)):
        a_ref[i] = nn(left, w_ref[i, :, :half]).astype(BF16)
        b_ref[i] = nn(left, w_ref[i, :, half:]).astype(BF16)


def forward(p, m, w, n_dp, n_z):
    slot_count = n_dp * n_z * CAP
    n, width, cols = w.shape
    part = pltpu.VMEM((n, slot_count, cols // 2), BF16)
    return pl.pallas_call(
        functools.partial(forward_kernel, n_dp=n_dp),
        out_shape=[pltpu.VMEM((2, slot_count, width), BF16), part, part],
        in_specs=[pl.BlockSpec(memory_space=SMEM)] + [pl.BlockSpec(memory_space=VMEM)] * 2,
        out_specs=[pl.BlockSpec(memory_space=VMEM)] * 3,
        compiler_params=pltpu.CompilerParams(vmem_limit_bytes=LIMIT),
        name="forward",
    )(p, m, w)


def backward_kernel(e_ref, a_ref, ra_ref, b_ref, rb_ref, w_ref, *refs, n_dp):
    g_ref, out_ref = refs[-2:]
    before_ref = refs[0] if len(refs) == 3 else None
    slot_count = g_ref.shape[1]
    group = slot_count // n_dp
    half = a_ref.shape[2]
    back = None
    for h, (u_ref, v_ref) in enumerate(((a_ref, ra_ref), (b_ref, rb_ref))):
        at = slice(h * half, (h + 1) * half)
        gate = u_ref[0].astype(F32) + v_ref[0].astype(F32)
        up = u_ref[1].astype(F32) + v_ref[1].astype(F32)
        down = u_ref[2].astype(F32) + v_ref[2].astype(F32)
        sig = jax.nn.sigmoid(gate)
        act = gate * sig
        gate_grad = (down * up * sig * (1.0 + gate * (1.0 - sig))).astype(BF16)
        up_grad = (down * act).astype(BF16)
        g_ref[0, :, at] = gate_grad
        g_ref[1, :, at] = up_grad
        g_ref[2, :, at] = (act * up).astype(BF16)
        part = nt(gate_grad, w_ref[0, :, at]) + nt(up_grad, w_ref[1, :, at])
        back = part if back is None else back + part
    back = back.astype(BF16)
    if before_ref is None:
        out_ref[...] = back
        return
    count, capp, _ = out_ref.shape
    n_ex = count // n_dp
    both = jnp.concatenate([before_ref[...], back], axis=0)
    o = lax.broadcasted_iota(I32, (count * capp, 1), 0)
    c = o & (capp - 1)
    ex = ((o >> log2(capp)) & (n_ex - 1)) ^ e_ref[0]
    pa = o >> (log2(capp) + log2(n_ex))
    slot = (ex & 1) * slot_count + pa * group + (ex >> 1) * CAP + c
    slot = jnp.where(c < CAP, slot, -1)
    hit = lax.broadcasted_iota(I32, (count * capp, CORES * slot_count), 1) == slot
    out = nn(jnp.where(hit, 1.0, 0.0).astype(BF16), both).astype(BF16)
    for d in range(count):
        out_ref[d] = out[d * capp : (d + 1) * capp]


def backward(e, a, ra, b, rb, w, n_dp, n_ex, before=()):
    n, slot_count, half = a.shape
    width = w.shape[1]
    shape = (n_dp * n_ex, CAPP, width) if before else (slot_count, width)
    return pl.pallas_call(
        functools.partial(backward_kernel, n_dp=n_dp),
        out_shape=[pltpu.VMEM((n, slot_count, 2 * half), BF16), pltpu.VMEM(shape, BF16)],
        in_specs=[pl.BlockSpec(memory_space=SMEM)]
        + [pl.BlockSpec(memory_space=VMEM)] * (5 + len(before)),
        out_specs=[pl.BlockSpec(memory_space=VMEM)] * 2,
        compiler_params=pltpu.CompilerParams(vmem_limit_bytes=LIMIT),
        name="backward",
    )(e, a, ra, b, rb, w, *before)


def weight_grad_kernel(*refs, planes, tile):
    x0_ref, x1_ref, g0_ref, g1_ref = refs[:4]
    out_ref, scratch, sem = refs[-3:]
    width = x0_ref.shape[2]
    copies = []
    for a in planes:
        x = jnp.concatenate([x0_ref[a // 2], x1_ref[a // 2]], axis=0)
        g = jnp.concatenate([g0_ref[a], g1_ref[a]], axis=0)
        for r in range(0, width, tile):
            i = len(copies)
            scratch[i] = tn(x[:, r : r + tile], g)
            copy = pltpu.make_async_copy(scratch.at[i], out_ref.at[a, pl.ds(r, tile)], sem.at[i])
            copy.start()
            copies.append(copy)
    for copy in copies:
        copy.wait()


def weight_grad(planes, x0, x1, g0, g1, total=None):
    n, _, cols = g0.shape
    width = x0.shape[2]
    tile = width // 3 if width % (3 * 128) == 0 else width
    steps = len(planes) * (width // tile)
    operands = [x0, x1, g0, g1] + ([] if total is None else [total])
    return pl.pallas_call(
        functools.partial(weight_grad_kernel, planes=planes, tile=tile),
        out_shape=pltpu.HBM((n, width, cols), F32),
        in_specs=[pl.BlockSpec(memory_space=VMEM)] * 4
        + [pl.BlockSpec(memory_space=pltpu.HBM)] * (len(operands) - 4),
        out_specs=pl.BlockSpec(memory_space=pltpu.HBM),
        scratch_shapes=[
            pltpu.VMEM((steps, tile, cols), F32),
            pltpu.SemaphoreType.DMA((steps,)),
        ],
        input_output_aliases={} if total is None else {4: 0},
        compiler_params=pltpu.CompilerParams(vmem_limit_bytes=LIMIT),
        name="weight_grad",
    )(*operands)


def place_kernel(hit_ref, got_ref, out_ref, *, n_dp):
    count, capp, width = got_ref.shape
    n_ex = count // n_dp
    hit = hit_ref[:capp, :].astype(BF16)
    for p in range(n_dp):
        total = got_ref[p * n_ex].astype(F32)
        for e in range(1, n_ex):
            total = total + got_ref[p * n_ex + e].astype(F32)
        out_ref[:, p * width : (p + 1) * width] = tn(hit, total.astype(BF16)).astype(BF16)


def place(hit, got, tok, n_dp):
    width = got.shape[2]
    return pl.pallas_call(
        functools.partial(place_kernel, n_dp=n_dp),
        out_shape=jax.ShapeDtypeStruct((tok, width * n_dp), BF16),
        in_specs=[pl.BlockSpec(memory_space=VMEM)] * 2,
        out_specs=pl.BlockSpec(memory_space=VMEM),
        compiler_params=pltpu.CompilerParams(vmem_limit_bytes=LIMIT),
        name="place",
    )(hit, got)


def add_bf16(u, v):
    return (u.astype(F32) + v.astype(F32)).astype(BF16)


def shift(x, axis, k):
    return lax.ppermute(x, axis, xor_pairs(lax.axis_size(axis), k))


def per_device_fast(out_grad, layer_input, expert_ids, gate_prob, w_stack, scale_exps):
    return fast_body(out_grad, layer_input, expert_ids, gate_prob, w_stack, scale_exps)


def fast_body(out_grad, layer_input, expert_ids, gate_prob, w_stack, scale_exps):
    n_dp = lax.axis_size("dp")
    n_ex = lax.axis_size("expert")
    n_z = n_ex // CORES
    tok = out_grad.shape[0]
    p = lax.axis_index("dp").astype(I32).reshape(1)
    e = lax.axis_index("expert").astype(I32).reshape(1)
    hit, *blocks = slots(p, e, expert_ids.T, gate_prob.T, out_grad, layer_input, n_dp)
    w = scale_weights(scale_exps, w_stack)
    got = [blocks[0]] + [shift(blocks[k], "dp", k) for k in range(1, n_dp)]
    mine = jnp.concatenate(got, axis=0)
    column = [mine] + [shift(mine, "expert", k * CORES) for k in range(1, n_z)]
    m0 = jnp.concatenate(column, axis=0)
    m1 = shift(m0, "expert", 1)
    xs, sums = [], []
    for m in (m0, m1):
        x, a, b = forward(p, m, w, n_dp, n_z)
        ra = shift(a, "dp", 1)
        rb = shift(b, "dp", 2)
        a = add_bf16(a, ra)
        b = add_bf16(b, rb)
        ra = shift(a, "dp", 2)
        rb = shift(b, "dp", 1)
        xs.append(x)
        sums.append((a, ra, b, rb))
    gs, out = [], ()
    for a, ra, b, rb in sums:
        g, *out = backward(e, a, ra, b, rb, w, n_dp, n_ex, out)
        gs.append(g)
    weight_grads = weight_grad((0, 1, 2), *xs, *gs)
    got = lax.all_to_all(out[0], ("dp", "expert"), split_axis=0, concat_axis=0, tiled=True)
    input_grad = place(hit, got, tok, n_dp)
    return input_grad, weight_grads


def per_device_any(out_grad, layer_input, expert_ids, gate_prob, w_stack, scale_exps):
    n_dp = lax.axis_size("dp")
    _, d_model = out_grad.shape
    routed = expert_ids == 0
    mask = jnp.any(routed, axis=1)
    prob = jnp.sum(jnp.where(routed, gate_prob, 0.0), axis=1)
    rank = jnp.cumsum(mask.astype(I32)) - 1
    hit = ((rank[None, :] == jnp.arange(CAP)[:, None]) & mask[None, :]).astype(BF16)
    slot_input = jnp.dot(hit, layer_input, preferred_element_type=F32)
    slot_prob = jnp.sum(hit.astype(F32) * prob[None, :], axis=1)
    slot_grad = slot_prob[:, None] * jnp.dot(hit, out_grad, preferred_element_type=F32)
    both = jnp.stack([slot_input, slot_grad]).astype(BF16)
    both = both.reshape(2, CAP, n_dp, d_model // n_dp).transpose(2, 0, 1, 3)
    both = lax.all_to_all(both, "dp", split_axis=0, concat_axis=0, tiled=True)
    both = lax.all_gather(both, "expert", axis=0)
    both = both.transpose(2, 0, 1, 3, 4)
    lead = both.shape[1:4]
    both = both.reshape(2, -1, both.shape[-1])
    n, rows, cols = w_stack.shape
    factor = jnp.exp2(scale_exps.astype(F32))
    tiles = factor.shape[1:]
    w = w_stack.astype(F32).reshape(n, tiles[0], rows // tiles[0], tiles[1], cols // tiles[1])
    w = (w * factor[:, :, None, :, None]).reshape(n, rows, cols).astype(BF16)
    sides = jnp.stack([both[0], both[0], both[1]])
    partial = jnp.einsum("nrk,nkh->nrh", sides, w, preferred_element_type=F32)
    gate, up, down = lax.psum(partial, "dp")
    sig = jax.nn.sigmoid(gate)
    act = gate * sig
    gate_grad = (down * up * sig * (1.0 + gate * (1.0 - sig))).astype(BF16)
    up_grad = (down * act).astype(BF16)
    hidden = (act * up).astype(BF16)
    back = nt(gate_grad, w[0]) + nt(up_grad, w[1])
    back = lax.psum_scatter(back.reshape(lead + (rows,)), "expert", scatter_dimension=0, tiled=False)
    back = lax.all_to_all(back, "dp", split_axis=0, concat_axis=0, tiled=True)
    back = back.transpose(1, 0, 2).reshape(CAP, d_model)
    input_grad = tn(hit, back.astype(BF16)).astype(BF16)
    weight_grads = jnp.einsum(
        "nrd,nrh->ndh", sides, jnp.stack([gate_grad, up_grad, hidden]), preferred_element_type=F32
    )
    return input_grad, weight_grads


def solution(mesh):
    n_dp, n_ex = mesh.shape["dp"], mesh.shape["expert"]
    n_z = n_ex // CORES
    fast = n_dp == 4 and n_ex % CORES == 0 and is_pow2(n_z) and n_z <= 4
    in_specs = (
        P(("dp", "expert"), None),
        P(("dp", "expert"), None),
        P(("dp", "expert"), None),
        P(("dp", "expert"), None),
        P(None, "dp", "expert"),
        P(None, "dp", "expert"),
    )
    out_specs = (P(("dp", "expert"), None), P(None, "dp", "expert"))
    return jax.shard_map(
        per_device_fast if fast else per_device_any,
        mesh=mesh,
        in_specs=in_specs,
        out_specs=out_specs,
        check_vma=False,
    )
```

```python
import functools

import jax
import jax.numpy as jnp
from jax import lax
from jax.experimental import pallas as pl
from jax.experimental.pallas import tpu as pltpu
from jax.sharding import PartitionSpec as P


CAP = 3
BF16 = jnp.bfloat16
F32 = jnp.float32
I32 = jnp.int32
ROWS = 8
CHUNKS = 3
CAPP = 2
CORES = 2
LIMIT = 20 * 1024 * 1024
VMEM = pltpu.VMEM
SMEM = pltpu.SMEM


def in_hbm(x):
    return pltpu.with_memory_space_constraint(x, pltpu.HBM)


def log2(n):
    return n.bit_length() - 1


def is_pow2(n):
    return n & (n - 1) == 0


def xor_pairs(n, k):
    return [(i, i ^ k) for i in range(n)]


def nn(a, b):
    return lax.dot_general(a, b, (((1,), (0,)), ((), ())), preferred_element_type=F32)


def nt(a, b):
    return lax.dot_general(a, b, (((1,), (1,)), ((), ())), preferred_element_type=F32)


def tn(a, b):
    return lax.dot_general(a, b, (((0,), (0,)), ((), ())), preferred_element_type=F32)


def slots_kernel(p_ref, e_ref, ids_hbm, prob_hbm, grad_hbm, inp_hbm, hit_ref, *refs):
    outs = refs[:-6]
    scratch, ids_ref, prob_ref, grad_ref, inp_ref, sem = refs[-6:]
    pairs = ((ids_hbm, ids_ref), (prob_hbm, prob_ref), (inp_hbm, inp_ref), (grad_hbm, grad_ref))
    copies = [pltpu.make_async_copy(u, v, sem.at[i]) for i, (u, v) in enumerate(pairs)]
    for copy in copies:
        copy.start()
    for copy in copies:
        copy.wait()
    n_dp = len(outs)
    width = outs[0].shape[1]
    tok = ids_ref.shape[1]
    named = ids_ref[...] == 0
    prob = jnp.sum(jnp.where(named, prob_ref[...], 0.0), axis=0, keepdims=True)
    routed = jnp.sum(named.astype(F32), axis=0, keepdims=True)
    earlier = lax.broadcasted_iota(I32, (tok, tok), 0) <= lax.broadcasted_iota(I32, (tok, tok), 1)
    rank = nn(jnp.broadcast_to(routed, (ROWS, tok)).astype(BF16), earlier.astype(BF16)) - 1.0
    row = lax.broadcasted_iota(I32, (ROWS, tok), 0)
    is_routed = jnp.broadcast_to(routed, (ROWS, tok)) > 0.5
    hit_in = is_routed & (rank == row.astype(F32))
    hit_gr = is_routed & (rank == (row - CAP).astype(F32))
    hit_in = jnp.where(hit_in & (row < CAP), 1.0, 0.0)
    hit_gr = jnp.where(hit_gr & (row >= CAP) & (row < 2 * CAP), 1.0, 0.0)
    slot_prob = jnp.sum(hit_gr * prob, axis=1, keepdims=True)
    hit_ref[...] = hit_in
    rows = nn(hit_in.astype(BF16), inp_ref[...]) + slot_prob * nn(hit_gr.astype(BF16), grad_ref[...])
    for d in range(n_dp):
        scratch[d] = rows[:, d * width : (d + 1) * width].astype(BF16)
    p = p_ref[0]
    for k in range(n_dp):
        outs[k][...] = scratch[p ^ k]


def slots(p, e, ids, prob, grad, inp, n_dp):
    tok, d_model = inp.shape
    width = d_model // n_dp
    return pl.pallas_call(
        slots_kernel,
        out_shape=[pltpu.VMEM((ROWS, tok), F32)] + [pltpu.VMEM((ROWS, width), BF16)] * n_dp,
        in_specs=[pl.BlockSpec(memory_space=SMEM)] * 2 + [pl.BlockSpec(memory_space=pltpu.HBM)] * 4,
        out_specs=[pl.BlockSpec(memory_space=VMEM)] * (n_dp + 1),
        scratch_shapes=[
            pltpu.VMEM((n_dp, ROWS, width), BF16),
            pltpu.VMEM(ids.shape, I32),
            pltpu.VMEM(prob.shape, F32),
            pltpu.VMEM(grad.shape, BF16),
            pltpu.VMEM(inp.shape, BF16),
            pltpu.SemaphoreType.DMA((4,)),
        ],
        compiler_params=pltpu.CompilerParams(vmem_limit_bytes=LIMIT),
        name="slots",
    )(p, e, *(in_hbm(v) for v in (ids, prob, grad, inp)))


def scale_kernel(exp_hbm, w_ref, out_ref, exp_ref, sem):
    exp_copy = pltpu.make_async_copy(exp_hbm, exp_ref, sem.at[sem.shape[0] - 1])
    exp_copy.start()
    n, rows, cols = w_ref.shape
    tile = rows // exp_ref.shape[1]
    chunk = rows // CHUNKS if exp_ref.shape[1] % CHUNKS == 0 else rows
    copies = []
    for a in range(n):
        for c in range(rows // chunk):
            at = (a, pl.ds(c * chunk, chunk))
            copies.append(
                pltpu.make_async_copy(w_ref.at[at], out_ref.at[at], sem.at[len(copies)])
            )
    for copy in copies:
        copy.start()
    exp_copy.wait()
    for step, copy in enumerate(copies):
        a, c = divmod(step, rows // chunk)
        copy.wait()
        for i in range(chunk // tile):
            for j in range(cols // tile):
                row = c * (chunk // tile) + i
                at = (a, slice(row * tile, (row + 1) * tile), slice(j * tile, (j + 1) * tile))
                e = exp_ref[a, row, j]
                factor = jnp.where(e > 0, 2.0, jnp.where(e < 0, 0.5, 1.0))
                out_ref[at] = out_ref[at] * factor.astype(BF16)


def scale_weights(exps, w):
    n, _, _ = w.shape
    return pl.pallas_call(
        scale_kernel,
        out_shape=pltpu.VMEM(w.shape, BF16),
        in_specs=[pl.BlockSpec(memory_space=pltpu.HBM)] * 2,
        out_specs=pl.BlockSpec(memory_space=VMEM),
        scratch_shapes=[
            pltpu.SMEM(exps.shape, I32),
            pltpu.SemaphoreType.DMA((n * CHUNKS + 1,)),
        ],
        compiler_params=pltpu.CompilerParams(vmem_limit_bytes=LIMIT),
        name="scale",
    )(in_hbm(exps), in_hbm(w))


def forward_kernel(p_ref, m_ref, w_ref, x_ref, a_ref, b_ref, *, n_dp):
    slot_count = x_ref.shape[1]
    group = slot_count // n_dp
    span = m_ref.shape[0]
    p = p_ref[0]
    col = lax.broadcasted_iota(I32, (1, span), 1)
    r = col & (ROWS - 1)
    pk = (col >> log2(ROWS)) & (n_dp - 1)
    zk = col >> (log2(ROWS) + log2(n_dp))
    line = lax.broadcasted_iota(I32, (slot_count, span), 0)

    def pick(low):
        slot = (p ^ pk) * group + zk * CAP + (r - low)
        slot = jnp.where((r >= low) & (r < low + CAP), slot, -1)
        sel = jnp.where(line == slot, 1.0, 0.0).astype(BF16)
        return nn(sel, m_ref[...]).astype(BF16)

    x = pick(0)
    g = pick(CAP)
    x_ref[0] = x
    x_ref[1] = g
    half = a_ref.shape[2]
    for i, left in enumerate((x, x, g)):
        a_ref[i] = nn(left, w_ref[i, :, :half]).astype(BF16)
        b_ref[i] = nn(left, w_ref[i, :, half:]).astype(BF16)


def forward(p, m, w, n_dp, n_z):
    slot_count = n_dp * n_z * CAP
    n, width, cols = w.shape
    part = pltpu.VMEM((n, slot_count, cols // 2), BF16)
    return pl.pallas_call(
        functools.partial(forward_kernel, n_dp=n_dp),
        out_shape=[pltpu.VMEM((2, slot_count, width), BF16), part, part],
        in_specs=[pl.BlockSpec(memory_space=SMEM)] + [pl.BlockSpec(memory_space=VMEM)] * 2,
        out_specs=[pl.BlockSpec(memory_space=VMEM)] * 3,
        compiler_params=pltpu.CompilerParams(vmem_limit_bytes=LIMIT),
        name="forward",
    )(p, m, w)


def backward_kernel(e_ref, a_ref, ra_ref, b_ref, rb_ref, w_ref, *refs, n_dp):
    g_ref, out_ref = refs[-2:]
    before_ref = refs[0] if len(refs) == 3 else None
    slot_count = g_ref.shape[1]
    group = slot_count // n_dp
    half = a_ref.shape[2]
    back = None
    for h, (u_ref, v_ref) in enumerate(((a_ref, ra_ref), (b_ref, rb_ref))):
        at = slice(h * half, (h + 1) * half)
        gate = u_ref[0].astype(F32) + v_ref[0].astype(F32)
        up = u_ref[1].astype(F32) + v_ref[1].astype(F32)
        down = u_ref[2].astype(F32) + v_ref[2].astype(F32)
        sig = jax.nn.sigmoid(gate)
        act = gate * sig
        gate_grad = (down * up * sig * (1.0 + gate * (1.0 - sig))).astype(BF16)
        up_grad = (down * act).astype(BF16)
        g_ref[0, :, at] = gate_grad
        g_ref[1, :, at] = up_grad
        g_ref[2, :, at] = (act * up).astype(BF16)
        part = nt(gate_grad, w_ref[0, :, at]) + nt(up_grad, w_ref[1, :, at])
        back = part if back is None else back + part
    back = back.astype(BF16)
    if before_ref is None:
        out_ref[...] = back
        return
    count, capp, lanes = out_ref.shape
    n_ex = count // n_dp
    part = lanes // CAP
    both = jnp.concatenate([before_ref[...], back], axis=0)
    o = lax.broadcasted_iota(I32, (count * capp, 1), 0)
    q = o & (capp - 1)
    ex = ((o >> log2(capp)) & (n_ex - 1)) ^ e_ref[0]
    pa = o >> (log2(capp) + log2(n_ex))
    slot = (ex & 1) * slot_count + pa * group + (ex >> 1) * CAP
    line = lax.broadcasted_iota(I32, (count * capp, CORES * slot_count), 1)
    for j in range(CAP):
        total = None
        for half in range(2):
            wanted = -1
            for row in range(capp):
                c, h = divmod(row * CAP + j, 2)
                if h == half:
                    wanted = jnp.where(q == row, slot + c, wanted)
            hit = jnp.where(line == wanted, 1.0, 0.0).astype(BF16)
            moved = nn(hit, both[:, half * part : (half + 1) * part])
            total = moved if total is None else total + moved
        total = total.astype(BF16)
        for d in range(count):
            out_ref[d, :, j * part : (j + 1) * part] = total[d * capp : (d + 1) * capp]


def backward(e, a, ra, b, rb, w, n_dp, n_ex, before=()):
    n, slot_count, half = a.shape
    width = w.shape[1]
    shape = (n_dp * n_ex, CAPP, width * CAP // CAPP) if before else (slot_count, width)
    return pl.pallas_call(
        functools.partial(backward_kernel, n_dp=n_dp),
        out_shape=[pltpu.VMEM((n, slot_count, 2 * half), BF16), pltpu.VMEM(shape, BF16)],
        in_specs=[pl.BlockSpec(memory_space=SMEM)]
        + [pl.BlockSpec(memory_space=VMEM)] * (5 + len(before)),
        out_specs=[pl.BlockSpec(memory_space=VMEM)] * 2,
        compiler_params=pltpu.CompilerParams(vmem_limit_bytes=LIMIT),
        name="backward",
    )(e, a, ra, b, rb, w, *before)


def weight_grad_kernel(*refs, planes, tile):
    x0_ref, x1_ref, g0_ref, g1_ref = refs[:4]
    out_ref, scratch, sem = refs[-3:]
    width = x0_ref.shape[2]
    copies = []
    for a in planes:
        x = jnp.concatenate([x0_ref[a // 2], x1_ref[a // 2]], axis=0)
        g = jnp.concatenate([g0_ref[a], g1_ref[a]], axis=0)
        for r in range(0, width, tile):
            i = len(copies)
            scratch[i] = tn(x[:, r : r + tile], g)
            copy = pltpu.make_async_copy(scratch.at[i], out_ref.at[a, pl.ds(r, tile)], sem.at[i])
            copy.start()
            copies.append(copy)
    for copy in copies:
        copy.wait()


def weight_grad(planes, x0, x1, g0, g1, total=None):
    n, _, cols = g0.shape
    width = x0.shape[2]
    tile = width // 3 if width % (3 * 128) == 0 else width
    steps = len(planes) * (width // tile)
    operands = [x0, x1, g0, g1] + ([] if total is None else [total])
    return pl.pallas_call(
        functools.partial(weight_grad_kernel, planes=planes, tile=tile),
        out_shape=pltpu.HBM((n, width, cols), F32),
        in_specs=[pl.BlockSpec(memory_space=VMEM)] * 4
        + [pl.BlockSpec(memory_space=pltpu.HBM)] * (len(operands) - 4),
        out_specs=pl.BlockSpec(memory_space=pltpu.HBM),
        scratch_shapes=[
            pltpu.VMEM((steps, tile, cols), F32),
            pltpu.SemaphoreType.DMA((steps,)),
        ],
        input_output_aliases={} if total is None else {4: 0},
        compiler_params=pltpu.CompilerParams(vmem_limit_bytes=LIMIT),
        name="weight_grad",
    )(*operands)


def place_kernel(hit_ref, got_ref, out_ref, *, n_dp):
    count, capp, lanes = got_ref.shape
    n_ex = count // n_dp
    part = lanes // CAP
    hit = hit_ref[...]
    row = lax.broadcasted_iota(I32, (capp, hit.shape[1]), 0)
    picks = []
    for half in range(2):
        for j in range(CAP):
            pick = jnp.zeros(row.shape, F32)
            for r in range(capp):
                c, h = divmod(r * CAP + j, 2)
                if h == half:
                    pick = jnp.where(row == r, hit[c : c + 1], pick)
            picks.append(pick.astype(BF16))
    for p in range(n_dp):
        total = got_ref[p * n_ex].astype(F32)
        for e in range(1, n_ex):
            total = total + got_ref[p * n_ex + e].astype(F32)
        total = total.astype(BF16)
        for half in range(2):
            out = None
            for j in range(CAP):
                moved = tn(picks[half * CAP + j], total[:, j * part : (j + 1) * part])
                out = moved if out is None else out + moved
            at = (2 * p + half) * part
            out_ref[:, at : at + part] = out.astype(BF16)


def place(hit, got, tok, n_dp):
    width = got.shape[2] // CAP * 2
    return pl.pallas_call(
        functools.partial(place_kernel, n_dp=n_dp),
        out_shape=jax.ShapeDtypeStruct((tok, width * n_dp), BF16),
        in_specs=[pl.BlockSpec(memory_space=VMEM)] * 2,
        out_specs=pl.BlockSpec(memory_space=VMEM),
        compiler_params=pltpu.CompilerParams(vmem_limit_bytes=LIMIT),
        name="place",
    )(hit, got)


def add_bf16(u, v):
    return (u.astype(F32) + v.astype(F32)).astype(BF16)


def shift(x, axis, k):
    return lax.ppermute(x, axis, xor_pairs(lax.axis_size(axis), k))


def per_device_fast(out_grad, layer_input, expert_ids, gate_prob, w_stack, scale_exps):
    return fast_body(out_grad, layer_input, expert_ids, gate_prob, w_stack, scale_exps)


def fast_body(out_grad, layer_input, expert_ids, gate_prob, w_stack, scale_exps):
    n_dp = lax.axis_size("dp")
    n_ex = lax.axis_size("expert")
    n_z = n_ex // CORES
    tok = out_grad.shape[0]
    p = lax.axis_index("dp").astype(I32).reshape(1)
    e = lax.axis_index("expert").astype(I32).reshape(1)
    hit, *blocks = slots(p, e, expert_ids.T, gate_prob.T, out_grad, layer_input, n_dp)
    w = scale_weights(scale_exps, w_stack)
    got = [blocks[0]] + [shift(blocks[k], "dp", k) for k in range(1, n_dp)]
    mine = jnp.concatenate(got, axis=0)
    column = [mine] + [shift(mine, "expert", k * CORES) for k in range(1, n_z)]
    m0 = jnp.concatenate(column, axis=0)
    m1 = shift(m0, "expert", 1)
    xs, sums = [], []
    for m in (m0, m1):
        x, a, b = forward(p, m, w, n_dp, n_z)
        ra = shift(a, "dp", 1)
        rb = shift(b, "dp", 2)
        a = add_bf16(a, ra)
        b = add_bf16(b, rb)
        ra = shift(a, "dp", 2)
        rb = shift(b, "dp", 1)
        xs.append(x)
        sums.append((a, ra, b, rb))
    gs, out = [], ()
    for a, ra, b, rb in sums:
        g, *out = backward(e, a, ra, b, rb, w, n_dp, n_ex, out)
        gs.append(g)
    weight_grads = weight_grad((0, 1, 2), *xs, *gs)
    got = lax.all_to_all(out[0], ("dp", "expert"), split_axis=0, concat_axis=0, tiled=True)
    input_grad = place(hit, got, tok, n_dp)
    return input_grad, weight_grads


def per_device_any(out_grad, layer_input, expert_ids, gate_prob, w_stack, scale_exps):
    n_dp = lax.axis_size("dp")
    _, d_model = out_grad.shape
    routed = expert_ids == 0
    mask = jnp.any(routed, axis=1)
    prob = jnp.sum(jnp.where(routed, gate_prob, 0.0), axis=1)
    rank = jnp.cumsum(mask.astype(I32)) - 1
    hit = ((rank[None, :] == jnp.arange(CAP)[:, None]) & mask[None, :]).astype(BF16)
    slot_input = jnp.dot(hit, layer_input, preferred_element_type=F32)
    slot_prob = jnp.sum(hit.astype(F32) * prob[None, :], axis=1)
    slot_grad = slot_prob[:, None] * jnp.dot(hit, out_grad, preferred_element_type=F32)
    both = jnp.stack([slot_input, slot_grad]).astype(BF16)
    both = both.reshape(2, CAP, n_dp, d_model // n_dp).transpose(2, 0, 1, 3)
    both = lax.all_to_all(both, "dp", split_axis=0, concat_axis=0, tiled=True)
    both = lax.all_gather(both, "expert", axis=0)
    both = both.transpose(2, 0, 1, 3, 4)
    lead = both.shape[1:4]
    both = both.reshape(2, -1, both.shape[-1])
    n, rows, cols = w_stack.shape
    factor = jnp.exp2(scale_exps.astype(F32))
    tiles = factor.shape[1:]
    w = w_stack.astype(F32).reshape(n, tiles[0], rows // tiles[0], tiles[1], cols // tiles[1])
    w = (w * factor[:, :, None, :, None]).reshape(n, rows, cols).astype(BF16)
    sides = jnp.stack([both[0], both[0], both[1]])
    partial = jnp.einsum("nrk,nkh->nrh", sides, w, preferred_element_type=F32)
    gate, up, down = lax.psum(partial, "dp")
    sig = jax.nn.sigmoid(gate)
    act = gate * sig
    gate_grad = (down * up * sig * (1.0 + gate * (1.0 - sig))).astype(BF16)
    up_grad = (down * act).astype(BF16)
    hidden = (act * up).astype(BF16)
    back = nt(gate_grad, w[0]) + nt(up_grad, w[1])
    back = lax.psum_scatter(back.reshape(lead + (rows,)), "expert", scatter_dimension=0, tiled=False)
    back = lax.all_to_all(back, "dp", split_axis=0, concat_axis=0, tiled=True)
    back = back.transpose(1, 0, 2).reshape(CAP, d_model)
    input_grad = tn(hit, back.astype(BF16)).astype(BF16)
    weight_grads = jnp.einsum(
        "nrd,nrh->ndh", sides, jnp.stack([gate_grad, up_grad, hidden]), preferred_element_type=F32
    )
    return input_grad, weight_grads


def solution(mesh):
    n_dp, n_ex = mesh.shape["dp"], mesh.shape["expert"]
    n_z = n_ex // CORES
    fast = n_dp == 4 and n_ex % CORES == 0 and is_pow2(n_z) and n_z <= 4
    in_specs = (
        P(("dp", "expert"), None),
        P(("dp", "expert"), None),
        P(("dp", "expert"), None),
        P(("dp", "expert"), None),
        P(None, "dp", "expert"),
        P(None, "dp", "expert"),
    )
    out_specs = (P(("dp", "expert"), None), P(None, "dp", "expert"))
    return jax.shard_map(
        per_device_fast if fast else per_device_any,
        mesh=mesh,
        in_specs=in_specs,
        out_specs=out_specs,
        check_vma=False,
    )
```

```python
import functools

import jax
import jax.numpy as jnp
from jax import lax
from jax.experimental import pallas as pl
from jax.experimental.pallas import tpu as pltpu
from jax.sharding import PartitionSpec as P


CAP = 3
BF16 = jnp.bfloat16
F32 = jnp.float32
I32 = jnp.int32
ROWS = 8
CHUNKS = 3
CAPP = 2
CORES = 2
LIMIT = 20 * 1024 * 1024
VMEM = pltpu.VMEM
SMEM = pltpu.SMEM


def in_hbm(x):
    return pltpu.with_memory_space_constraint(x, pltpu.HBM)


def log2(n):
    return n.bit_length() - 1


def is_pow2(n):
    return n & (n - 1) == 0


def xor_pairs(n, k):
    return [(i, i ^ k) for i in range(n)]


def nn(a, b):
    return lax.dot_general(a, b, (((1,), (0,)), ((), ())), preferred_element_type=F32)


def nt(a, b):
    return lax.dot_general(a, b, (((1,), (1,)), ((), ())), preferred_element_type=F32)


def tn(a, b):
    return lax.dot_general(a, b, (((0,), (0,)), ((), ())), preferred_element_type=F32)


def slots_kernel(p_ref, e_ref, ids_hbm, prob_hbm, grad_hbm, inp_hbm, hit_ref, *refs):
    outs = refs[:-6]
    scratch, ids_ref, prob_ref, grad_ref, inp_ref, sem = refs[-6:]
    pairs = ((ids_hbm, ids_ref), (prob_hbm, prob_ref), (inp_hbm, inp_ref), (grad_hbm, grad_ref))
    copies = [pltpu.make_async_copy(u, v, sem.at[i]) for i, (u, v) in enumerate(pairs)]
    for copy in copies:
        copy.start()
    copies[0].wait()
    copies[1].wait()
    n_dp = len(outs)
    width = outs[0].shape[1]
    tok = ids_ref.shape[1]
    named = ids_ref[...] == 0
    prob = jnp.sum(jnp.where(named, prob_ref[...], 0.0), axis=0, keepdims=True)
    routed = jnp.sum(named.astype(F32), axis=0, keepdims=True)
    earlier = lax.broadcasted_iota(I32, (tok, tok), 0) <= lax.broadcasted_iota(I32, (tok, tok), 1)
    rank = nn(jnp.broadcast_to(routed, (ROWS, tok)).astype(BF16), earlier.astype(BF16)) - 1.0
    row = lax.broadcasted_iota(I32, (ROWS, tok), 0)
    is_routed = jnp.broadcast_to(routed, (ROWS, tok)) > 0.5
    hit_in = is_routed & (rank == row.astype(F32))
    hit_gr = is_routed & (rank == (row - CAP).astype(F32))
    hit_in = jnp.where(hit_in & (row < CAP), 1.0, 0.0)
    hit_gr = jnp.where(hit_gr & (row >= CAP) & (row < 2 * CAP), 1.0, 0.0)
    slot_prob = jnp.sum(hit_gr * prob, axis=1, keepdims=True)
    hit_ref[...] = hit_in
    copies[2].wait()
    copies[3].wait()
    rows = nn(hit_in.astype(BF16), inp_ref[...]) + slot_prob * nn(hit_gr.astype(BF16), grad_ref[...])
    for d in range(n_dp):
        scratch[d] = rows[:, d * width : (d + 1) * width].astype(BF16)
    p = p_ref[0]
    for k in range(n_dp):
        outs[k][...] = scratch[p ^ k]


def slots(p, e, ids, prob, grad, inp, n_dp):
    tok, d_model = inp.shape
    width = d_model // n_dp
    return pl.pallas_call(
        slots_kernel,
        out_shape=[pltpu.VMEM((ROWS, tok), F32)] + [pltpu.VMEM((ROWS, width), BF16)] * n_dp,
        in_specs=[pl.BlockSpec(memory_space=SMEM)] * 2 + [pl.BlockSpec(memory_space=pltpu.HBM)] * 4,
        out_specs=[pl.BlockSpec(memory_space=VMEM)] * (n_dp + 1),
        scratch_shapes=[
            pltpu.VMEM((n_dp, ROWS, width), BF16),
            pltpu.VMEM(ids.shape, I32),
            pltpu.VMEM(prob.shape, F32),
            pltpu.VMEM(grad.shape, BF16),
            pltpu.VMEM(inp.shape, BF16),
            pltpu.SemaphoreType.DMA((4,)),
        ],
        compiler_params=pltpu.CompilerParams(vmem_limit_bytes=LIMIT),
        name="slots",
    )(p, e, *(in_hbm(v) for v in (ids, prob, grad, inp)))


def scale_kernel(exp_hbm, w_ref, out_ref, exp_ref, sem):
    exp_copy = pltpu.make_async_copy(exp_hbm, exp_ref, sem.at[sem.shape[0] - 1])
    exp_copy.start()
    n, rows, cols = w_ref.shape
    tile = rows // exp_ref.shape[1]
    chunk = rows // CHUNKS if exp_ref.shape[1] % CHUNKS == 0 else rows
    copies = []
    for a in range(n):
        for c in range(rows // chunk):
            at = (a, pl.ds(c * chunk, chunk))
            copies.append(
                pltpu.make_async_copy(w_ref.at[at], out_ref.at[at], sem.at[len(copies)])
            )
    for copy in copies:
        copy.start()
    exp_copy.wait()
    for step, copy in enumerate(copies):
        a, c = divmod(step, rows // chunk)
        copy.wait()
        for i in range(chunk // tile):
            for j in range(cols // tile):
                row = c * (chunk // tile) + i
                at = (a, slice(row * tile, (row + 1) * tile), slice(j * tile, (j + 1) * tile))
                e = exp_ref[a, row, j]
                factor = jnp.where(e > 0, 2.0, jnp.where(e < 0, 0.5, 1.0))
                out_ref[at] = out_ref[at] * factor.astype(BF16)


def scale_weights(exps, w):
    n, _, _ = w.shape
    return pl.pallas_call(
        scale_kernel,
        out_shape=pltpu.VMEM(w.shape, BF16),
        in_specs=[pl.BlockSpec(memory_space=pltpu.HBM)] * 2,
        out_specs=pl.BlockSpec(memory_space=VMEM),
        scratch_shapes=[
            pltpu.SMEM(exps.shape, I32),
            pltpu.SemaphoreType.DMA((n * CHUNKS + 1,)),
        ],
        compiler_params=pltpu.CompilerParams(vmem_limit_bytes=LIMIT),
        name="scale",
    )(in_hbm(exps), in_hbm(w))


def forward_kernel(p_ref, m_ref, w_ref, x_ref, a_ref, b_ref, *, n_dp):
    slot_count = x_ref.shape[1]
    group = slot_count // n_dp
    span = m_ref.shape[0]
    p = p_ref[0]
    col = lax.broadcasted_iota(I32, (1, span), 1)
    r = col & (ROWS - 1)
    pk = (col >> log2(ROWS)) & (n_dp - 1)
    zk = col >> (log2(ROWS) + log2(n_dp))
    line = lax.broadcasted_iota(I32, (slot_count, span), 0)

    def pick(low):
        slot = (p ^ pk) * group + zk * CAP + (r - low)
        slot = jnp.where((r >= low) & (r < low + CAP), slot, -1)
        sel = jnp.where(line == slot, 1.0, 0.0).astype(BF16)
        return nn(sel, m_ref[...]).astype(BF16)

    x = pick(0)
    g = pick(CAP)
    x_ref[0] = x
    x_ref[1] = g
    half = a_ref.shape[2]
    for i, left in enumerate((x, x, g)):
        a_ref[i] = nn(left, w_ref[i, :, :half]).astype(BF16)
        b_ref[i] = nn(left, w_ref[i, :, half:]).astype(BF16)


def forward(p, m, w, n_dp, n_z):
    slot_count = n_dp * n_z * CAP
    n, width, cols = w.shape
    part = pltpu.VMEM((n, slot_count, cols // 2), BF16)
    return pl.pallas_call(
        functools.partial(forward_kernel, n_dp=n_dp),
        out_shape=[pltpu.VMEM((2, slot_count, width), BF16), part, part],
        in_specs=[pl.BlockSpec(memory_space=SMEM)] + [pl.BlockSpec(memory_space=VMEM)] * 2,
        out_specs=[pl.BlockSpec(memory_space=VMEM)] * 3,
        compiler_params=pltpu.CompilerParams(vmem_limit_bytes=LIMIT),
        name="forward",
    )(p, m, w)


def backward_kernel(e_ref, a_ref, ra_ref, b_ref, rb_ref, w_ref, *refs, n_dp):
    g_ref, out_ref = refs[-2:]
    before_ref = refs[0] if len(refs) == 3 else None
    slot_count = g_ref.shape[1]
    group = slot_count // n_dp
    half = a_ref.shape[2]
    back = None
    for h, (u_ref, v_ref) in enumerate(((a_ref, ra_ref), (b_ref, rb_ref))):
        at = slice(h * half, (h + 1) * half)
        gate = u_ref[0].astype(F32) + v_ref[0].astype(F32)
        up = u_ref[1].astype(F32) + v_ref[1].astype(F32)
        down = u_ref[2].astype(F32) + v_ref[2].astype(F32)
        sig = jax.nn.sigmoid(gate)
        act = gate * sig
        gate_grad = (down * up * sig * (1.0 + gate * (1.0 - sig))).astype(BF16)
        up_grad = (down * act).astype(BF16)
        g_ref[0, :, at] = gate_grad
        g_ref[1, :, at] = up_grad
        g_ref[2, :, at] = (act * up).astype(BF16)
        part = nt(gate_grad, w_ref[0, :, at]) + nt(up_grad, w_ref[1, :, at])
        back = part if back is None else back + part
    back = back.astype(BF16)
    if before_ref is None:
        out_ref[...] = back
        return
    count, capp, lanes = out_ref.shape
    n_ex = count // n_dp
    part = lanes // CAP
    both = jnp.concatenate([before_ref[...], back], axis=0)
    o = lax.broadcasted_iota(I32, (count * capp, 1), 0)
    q = o & (capp - 1)
    ex = ((o >> log2(capp)) & (n_ex - 1)) ^ e_ref[0]
    pa = o >> (log2(capp) + log2(n_ex))
    slot = (ex & 1) * slot_count + pa * group + (ex >> 1) * CAP
    line = lax.broadcasted_iota(I32, (count * capp, CORES * slot_count), 1)
    for j in range(CAP):
        total = None
        for half in range(2):
            wanted = -1
            for row in range(capp):
                c, h = divmod(row * CAP + j, 2)
                if h == half:
                    wanted = jnp.where(q == row, slot + c, wanted)
            hit = jnp.where(line == wanted, 1.0, 0.0).astype(BF16)
            moved = nn(hit, both[:, half * part : (half + 1) * part])
            total = moved if total is None else total + moved
        total = total.astype(BF16)
        for d in range(count):
            out_ref[d, :, j * part : (j + 1) * part] = total[d * capp : (d + 1) * capp]


def backward(e, a, ra, b, rb, w, n_dp, n_ex, before=()):
    n, slot_count, half = a.shape
    width = w.shape[1]
    shape = (n_dp * n_ex, CAPP, width * CAP // CAPP) if before else (slot_count, width)
    return pl.pallas_call(
        functools.partial(backward_kernel, n_dp=n_dp),
        out_shape=[pltpu.VMEM((n, slot_count, 2 * half), BF16), pltpu.VMEM(shape, BF16)],
        in_specs=[pl.BlockSpec(memory_space=SMEM)]
        + [pl.BlockSpec(memory_space=VMEM)] * (5 + len(before)),
        out_specs=[pl.BlockSpec(memory_space=VMEM)] * 2,
        compiler_params=pltpu.CompilerParams(vmem_limit_bytes=LIMIT),
        name="backward",
    )(e, a, ra, b, rb, w, *before)


def weight_grad_kernel(*refs, planes, tile):
    x0_ref, x1_ref, g0_ref, g1_ref = refs[:4]
    out_ref, scratch, sem = refs[-3:]
    width = x0_ref.shape[2]
    copies = []
    for a in planes:
        x = jnp.concatenate([x0_ref[a // 2], x1_ref[a // 2]], axis=0)
        g = jnp.concatenate([g0_ref[a], g1_ref[a]], axis=0)
        for r in range(0, width, tile):
            i = len(copies)
            scratch[i] = tn(x[:, r : r + tile], g)
            copy = pltpu.make_async_copy(scratch.at[i], out_ref.at[a, pl.ds(r, tile)], sem.at[i])
            copy.start()
            copies.append(copy)
    for copy in copies:
        copy.wait()


def weight_grad(planes, x0, x1, g0, g1, total=None):
    n, _, cols = g0.shape
    width = x0.shape[2]
    tile = width // 3 if width % (3 * 128) == 0 else width
    steps = len(planes) * (width // tile)
    operands = [x0, x1, g0, g1] + ([] if total is None else [total])
    return pl.pallas_call(
        functools.partial(weight_grad_kernel, planes=planes, tile=tile),
        out_shape=pltpu.HBM((n, width, cols), F32),
        in_specs=[pl.BlockSpec(memory_space=VMEM)] * 4
        + [pl.BlockSpec(memory_space=pltpu.HBM)] * (len(operands) - 4),
        out_specs=pl.BlockSpec(memory_space=pltpu.HBM),
        scratch_shapes=[
            pltpu.VMEM((steps, tile, cols), F32),
            pltpu.SemaphoreType.DMA((steps,)),
        ],
        input_output_aliases={} if total is None else {4: 0},
        compiler_params=pltpu.CompilerParams(vmem_limit_bytes=LIMIT),
        name="weight_grad",
    )(*operands)


def place_kernel(hit_ref, got_ref, out_hbm, out_ref, sem, *, n_dp):
    copies = []
    count, capp, lanes = got_ref.shape
    n_ex = count // n_dp
    part = lanes // CAP
    hit = hit_ref[...]
    row = lax.broadcasted_iota(I32, (capp, hit.shape[1]), 0)
    picks = []
    for half in range(2):
        for j in range(CAP):
            pick = jnp.zeros(row.shape, F32)
            for r in range(capp):
                c, h = divmod(r * CAP + j, 2)
                if h == half:
                    pick = jnp.where(row == r, hit[c : c + 1], pick)
            picks.append(pick.astype(BF16))
    for p in range(n_dp):
        total = got_ref[p * n_ex].astype(F32)
        for e in range(1, n_ex):
            total = total + got_ref[p * n_ex + e].astype(F32)
        total = total.astype(BF16)
        for half in range(2):
            out = None
            for j in range(CAP):
                moved = tn(picks[half * CAP + j], total[:, j * part : (j + 1) * part])
                out = moved if out is None else out + moved
            at = (2 * p + half) * part
            out_ref[:, at : at + part] = out.astype(BF16)
        at = pl.ds(2 * p * part, 2 * part)
        copies.append(pltpu.make_async_copy(out_ref.at[:, at], out_hbm.at[:, at], sem.at[p]))
        copies[-1].start()
    for copy in copies:
        copy.wait()


def place(hit, got, tok, n_dp):
    width = got.shape[2] // CAP * 2
    return pl.pallas_call(
        functools.partial(place_kernel, n_dp=n_dp),
        out_shape=pltpu.HBM((tok, width * n_dp), BF16),
        in_specs=[pl.BlockSpec(memory_space=VMEM)] * 2,
        out_specs=pl.BlockSpec(memory_space=pltpu.HBM),
        scratch_shapes=[pltpu.VMEM((tok, width * n_dp), BF16), pltpu.SemaphoreType.DMA((n_dp,))],
        compiler_params=pltpu.CompilerParams(vmem_limit_bytes=LIMIT),
        name="place",
    )(hit, got)


def add_bf16(u, v):
    return (u.astype(F32) + v.astype(F32)).astype(BF16)


def shift(x, axis, k):
    return lax.ppermute(x, axis, xor_pairs(lax.axis_size(axis), k))


def per_device_fast(out_grad, layer_input, expert_ids, gate_prob, w_stack, scale_exps):
    return fast_body(out_grad, layer_input, expert_ids, gate_prob, w_stack, scale_exps)


def fast_body(out_grad, layer_input, expert_ids, gate_prob, w_stack, scale_exps):
    n_dp = lax.axis_size("dp")
    n_ex = lax.axis_size("expert")
    n_z = n_ex // CORES
    tok = out_grad.shape[0]
    p = lax.axis_index("dp").astype(I32).reshape(1)
    e = lax.axis_index("expert").astype(I32).reshape(1)
    hit, *blocks = slots(p, e, expert_ids.T, gate_prob.T, out_grad, layer_input, n_dp)
    w = scale_weights(scale_exps, w_stack)
    got = [blocks[0]] + [shift(blocks[k], "dp", k) for k in range(1, n_dp)]
    mine = jnp.concatenate(got, axis=0)
    column = [mine] + [shift(mine, "expert", k * CORES) for k in range(1, n_z)]
    m0 = jnp.concatenate(column, axis=0)
    m1 = shift(m0, "expert", 1)
    xs, sums = [], []
    for m in (m0, m1):
        x, a, b = forward(p, m, w, n_dp, n_z)
        ra = shift(a, "dp", 1)
        rb = shift(b, "dp", 2)
        a = add_bf16(a, ra)
        b = add_bf16(b, rb)
        ra = shift(a, "dp", 2)
        rb = shift(b, "dp", 1)
        xs.append(x)
        sums.append((a, ra, b, rb))
    gs, out = [], ()
    for a, ra, b, rb in sums:
        g, *out = backward(e, a, ra, b, rb, w, n_dp, n_ex, out)
        gs.append(g)
    weight_grads = weight_grad((0, 1, 2), *xs, *gs)
    got = lax.all_to_all(out[0], ("dp", "expert"), split_axis=0, concat_axis=0, tiled=True)
    input_grad = place(hit, got, tok, n_dp)
    return input_grad, weight_grads


def per_device_any(out_grad, layer_input, expert_ids, gate_prob, w_stack, scale_exps):
    n_dp = lax.axis_size("dp")
    _, d_model = out_grad.shape
    routed = expert_ids == 0
    mask = jnp.any(routed, axis=1)
    prob = jnp.sum(jnp.where(routed, gate_prob, 0.0), axis=1)
    rank = jnp.cumsum(mask.astype(I32)) - 1
    hit = ((rank[None, :] == jnp.arange(CAP)[:, None]) & mask[None, :]).astype(BF16)
    slot_input = jnp.dot(hit, layer_input, preferred_element_type=F32)
    slot_prob = jnp.sum(hit.astype(F32) * prob[None, :], axis=1)
    slot_grad = slot_prob[:, None] * jnp.dot(hit, out_grad, preferred_element_type=F32)
    both = jnp.stack([slot_input, slot_grad]).astype(BF16)
    both = both.reshape(2, CAP, n_dp, d_model // n_dp).transpose(2, 0, 1, 3)
    both = lax.all_to_all(both, "dp", split_axis=0, concat_axis=0, tiled=True)
    both = lax.all_gather(both, "expert", axis=0)
    both = both.transpose(2, 0, 1, 3, 4)
    lead = both.shape[1:4]
    both = both.reshape(2, -1, both.shape[-1])
    n, rows, cols = w_stack.shape
    factor = jnp.exp2(scale_exps.astype(F32))
    tiles = factor.shape[1:]
    w = w_stack.astype(F32).reshape(n, tiles[0], rows // tiles[0], tiles[1], cols // tiles[1])
    w = (w * factor[:, :, None, :, None]).reshape(n, rows, cols).astype(BF16)
    sides = jnp.stack([both[0], both[0], both[1]])
    partial = jnp.einsum("nrk,nkh->nrh", sides, w, preferred_element_type=F32)
    gate, up, down = lax.psum(partial, "dp")
    sig = jax.nn.sigmoid(gate)
    act = gate * sig
    gate_grad = (down * up * sig * (1.0 + gate * (1.0 - sig))).astype(BF16)
    up_grad = (down * act).astype(BF16)
    hidden = (act * up).astype(BF16)
    back = nt(gate_grad, w[0]) + nt(up_grad, w[1])
    back = lax.psum_scatter(back.reshape(lead + (rows,)), "expert", scatter_dimension=0, tiled=False)
    back = lax.all_to_all(back, "dp", split_axis=0, concat_axis=0, tiled=True)
    back = back.transpose(1, 0, 2).reshape(CAP, d_model)
    input_grad = tn(hit, back.astype(BF16)).astype(BF16)
    weight_grads = jnp.einsum(
        "nrd,nrh->ndh", sides, jnp.stack([gate_grad, up_grad, hidden]), preferred_element_type=F32
    )
    return input_grad, weight_grads


def solution(mesh):
    n_dp, n_ex = mesh.shape["dp"], mesh.shape["expert"]
    n_z = n_ex // CORES
    fast = n_dp == 4 and n_ex % CORES == 0 and is_pow2(n_z) and n_z <= 4
    in_specs = (
        P(("dp", "expert"), None),
        P(("dp", "expert"), None),
        P(("dp", "expert"), None),
        P(("dp", "expert"), None),
        P(None, "dp", "expert"),
        P(None, "dp", "expert"),
    )
    out_specs = (P(("dp", "expert"), None), P(None, "dp", "expert"))
    return jax.shard_map(
        per_device_fast if fast else per_device_any,
        mesh=mesh,
        in_specs=in_specs,
        out_specs=out_specs,
        check_vma=False,
    )
```

```python
import functools

import jax
import jax.numpy as jnp
from jax import lax
from jax.experimental import pallas as pl
from jax.experimental.pallas import tpu as pltpu
from jax.sharding import PartitionSpec as P


CAP = 3
BF16 = jnp.bfloat16
F32 = jnp.float32
I32 = jnp.int32
ROWS = 8
CHUNKS = 3
CAPP = 2
CORES = 2
LIMIT = 20 * 1024 * 1024
VMEM = pltpu.VMEM
SMEM = pltpu.SMEM


def in_hbm(x):
    return pltpu.with_memory_space_constraint(x, pltpu.HBM)


def log2(n):
    return n.bit_length() - 1


def is_pow2(n):
    return n & (n - 1) == 0


def xor_pairs(n, k):
    return [(i, i ^ k) for i in range(n)]


def nn(a, b):
    return lax.dot_general(a, b, (((1,), (0,)), ((), ())), preferred_element_type=F32)


def nt(a, b):
    return lax.dot_general(a, b, (((1,), (1,)), ((), ())), preferred_element_type=F32)


def tn(a, b):
    return lax.dot_general(a, b, (((0,), (0,)), ((), ())), preferred_element_type=F32)


def slots_kernel(p_ref, e_ref, ids_hbm, prob_hbm, grad_hbm, inp_hbm, hit_ref, *refs):
    outs = refs[:-6]
    scratch, ids_ref, prob_ref, grad_ref, inp_ref, sem = refs[-6:]
    pairs = ((ids_hbm, ids_ref), (prob_hbm, prob_ref), (inp_hbm, inp_ref), (grad_hbm, grad_ref))
    copies = [pltpu.make_async_copy(u, v, sem.at[i]) for i, (u, v) in enumerate(pairs)]
    for copy in copies:
        copy.start()
    copies[0].wait()
    copies[1].wait()
    n_dp = len(outs)
    width = outs[0].shape[1]
    tok = ids_ref.shape[1]
    named = ids_ref[...] == 0
    prob = jnp.sum(jnp.where(named, prob_ref[...], 0.0), axis=0, keepdims=True)
    routed = jnp.sum(named.astype(F32), axis=0, keepdims=True)
    earlier = lax.broadcasted_iota(I32, (tok, tok), 0) <= lax.broadcasted_iota(I32, (tok, tok), 1)
    rank = nn(jnp.broadcast_to(routed, (ROWS, tok)).astype(BF16), earlier.astype(BF16)) - 1.0
    row = lax.broadcasted_iota(I32, (ROWS, tok), 0)
    is_routed = jnp.broadcast_to(routed, (ROWS, tok)) > 0.5
    hit_in = is_routed & (rank == row.astype(F32))
    hit_gr = is_routed & (rank == (row - CAP).astype(F32))
    hit_in = jnp.where(hit_in & (row < CAP), 1.0, 0.0)
    hit_gr = jnp.where(hit_gr & (row >= CAP) & (row < 2 * CAP), 1.0, 0.0)
    slot_prob = jnp.sum(hit_gr * prob, axis=1, keepdims=True)
    hit_ref[...] = hit_in
    copies[2].wait()
    copies[3].wait()
    rows = nn(hit_in.astype(BF16), inp_ref[...]) + slot_prob * nn(hit_gr.astype(BF16), grad_ref[...])
    for d in range(n_dp):
        scratch[d] = rows[:, d * width : (d + 1) * width].astype(BF16)
    p = p_ref[0]
    for k in range(n_dp):
        outs[k][...] = scratch[p ^ k]


def slots(p, e, ids, prob, grad, inp, n_dp):
    tok, d_model = inp.shape
    width = d_model // n_dp
    return pl.pallas_call(
        slots_kernel,
        out_shape=[pltpu.VMEM((ROWS, tok), F32)] + [pltpu.VMEM((ROWS, width), BF16)] * n_dp,
        in_specs=[pl.BlockSpec(memory_space=SMEM)] * 2 + [pl.BlockSpec(memory_space=pltpu.HBM)] * 4,
        out_specs=[pl.BlockSpec(memory_space=VMEM)] * (n_dp + 1),
        scratch_shapes=[
            pltpu.VMEM((n_dp, ROWS, width), BF16),
            pltpu.VMEM(ids.shape, I32),
            pltpu.VMEM(prob.shape, F32),
            pltpu.VMEM(grad.shape, BF16),
            pltpu.VMEM(inp.shape, BF16),
            pltpu.SemaphoreType.DMA((4,)),
        ],
        compiler_params=pltpu.CompilerParams(vmem_limit_bytes=LIMIT),
        name="slots",
    )(p, e, *(in_hbm(v) for v in (ids, prob, grad, inp)))


def scale_kernel(exp_hbm, w_ref, out_ref, exp_ref, sem):
    exp_copy = pltpu.make_async_copy(exp_hbm, exp_ref, sem.at[sem.shape[0] - 1])
    exp_copy.start()
    n, rows, cols = w_ref.shape
    tile = rows // exp_ref.shape[1]
    chunk = rows // CHUNKS if exp_ref.shape[1] % CHUNKS == 0 else rows
    copies = []
    for a in range(n):
        for c in range(rows // chunk):
            at = (a, pl.ds(c * chunk, chunk))
            copies.append(
                pltpu.make_async_copy(w_ref.at[at], out_ref.at[at], sem.at[len(copies)])
            )
    for copy in copies:
        copy.start()
    exp_copy.wait()
    for step, copy in enumerate(copies):
        a, c = divmod(step, rows // chunk)
        copy.wait()
        for i in range(chunk // tile):
            for j in range(cols // tile):
                row = c * (chunk // tile) + i
                at = (a, slice(row * tile, (row + 1) * tile), slice(j * tile, (j + 1) * tile))
                e = exp_ref[a, row, j]
                factor = jnp.where(e > 0, 2.0, jnp.where(e < 0, 0.5, 1.0))
                out_ref[at] = out_ref[at] * factor.astype(BF16)


def scale_weights(exps, w):
    n, _, _ = w.shape
    return pl.pallas_call(
        scale_kernel,
        out_shape=pltpu.VMEM(w.shape, BF16),
        in_specs=[pl.BlockSpec(memory_space=pltpu.HBM)] * 2,
        out_specs=pl.BlockSpec(memory_space=VMEM),
        scratch_shapes=[
            pltpu.SMEM(exps.shape, I32),
            pltpu.SemaphoreType.DMA((n * CHUNKS + 1,)),
        ],
        compiler_params=pltpu.CompilerParams(vmem_limit_bytes=LIMIT),
        name="scale",
    )(in_hbm(exps), in_hbm(w))


def forward_kernel(p_ref, m_ref, w_ref, x_ref, a_ref, b_ref, *, n_dp):
    slot_count = x_ref.shape[1]
    group = slot_count // n_dp
    span = m_ref.shape[0]
    p = p_ref[0]
    col = lax.broadcasted_iota(I32, (1, span), 1)
    r = col & (ROWS - 1)
    pk = (col >> log2(ROWS)) & (n_dp - 1)
    zk = col >> (log2(ROWS) + log2(n_dp))
    line = lax.broadcasted_iota(I32, (slot_count, span), 0)

    def pick(low):
        slot = (p ^ pk) * group + zk * CAP + (r - low)
        slot = jnp.where((r >= low) & (r < low + CAP), slot, -1)
        sel = jnp.where(line == slot, 1.0, 0.0).astype(BF16)
        return nn(sel, m_ref[...]).astype(BF16)

    x = pick(0)
    g = pick(CAP)
    x_ref[0] = x
    x_ref[1] = g
    half = a_ref.shape[2]
    for i, left in enumerate((x, x, g)):
        a_ref[i] = nn(left, w_ref[i, :, :half]).astype(BF16)
        b_ref[i] = nn(left, w_ref[i, :, half:]).astype(BF16)


def forward(p, m, w, n_dp, n_z):
    slot_count = n_dp * n_z * CAP
    n, width, cols = w.shape
    part = pltpu.VMEM((n, slot_count, cols // 2), BF16)
    return pl.pallas_call(
        functools.partial(forward_kernel, n_dp=n_dp),
        out_shape=[pltpu.VMEM((2, slot_count, width), BF16), part, part],
        in_specs=[pl.BlockSpec(memory_space=SMEM)] + [pl.BlockSpec(memory_space=VMEM)] * 2,
        out_specs=[pl.BlockSpec(memory_space=VMEM)] * 3,
        compiler_params=pltpu.CompilerParams(vmem_limit_bytes=LIMIT),
        name="forward",
    )(p, m, w)


def backward_kernel(e_ref, a_ref, ra_ref, b_ref, rb_ref, w_ref, *refs, n_dp):
    g_ref, out_ref = refs[-2:]
    before_ref = refs[0] if len(refs) == 3 else None
    slot_count = g_ref.shape[1]
    group = slot_count // n_dp
    half = a_ref.shape[2]
    back = None
    for h, (u_ref, v_ref) in enumerate(((a_ref, ra_ref), (b_ref, rb_ref))):
        at = slice(h * half, (h + 1) * half)
        gate = u_ref[0].astype(F32) + v_ref[0].astype(F32)
        up = u_ref[1].astype(F32) + v_ref[1].astype(F32)
        down = u_ref[2].astype(F32) + v_ref[2].astype(F32)
        sig = jax.nn.sigmoid(gate)
        act = gate * sig
        gate_grad = (down * up * sig * (1.0 + gate * (1.0 - sig))).astype(BF16)
        up_grad = (down * act).astype(BF16)
        g_ref[0, :, at] = gate_grad
        g_ref[1, :, at] = up_grad
        g_ref[2, :, at] = (act * up).astype(BF16)
        part = nt(gate_grad, w_ref[0, :, at]) + nt(up_grad, w_ref[1, :, at])
        back = part if back is None else back + part
    back = back.astype(BF16)
    if before_ref is None:
        out_ref[...] = back
        return
    count, capp, lanes = out_ref.shape
    n_ex = count // n_dp
    part = lanes // CAP
    both = jnp.concatenate([before_ref[...], back], axis=0)
    o = lax.broadcasted_iota(I32, (count * capp, 1), 0)
    q = o & (capp - 1)
    ex = ((o >> log2(capp)) & (n_ex - 1)) ^ e_ref[0]
    pa = o >> (log2(capp) + log2(n_ex))
    slot = (ex & 1) * slot_count + pa * group + (ex >> 1) * CAP
    line = lax.broadcasted_iota(I32, (count * capp, CORES * slot_count), 1)
    for j in range(CAP):
        total = None
        for half in range(2):
            wanted = -1
            for row in range(capp):
                c, h = divmod(row * CAP + j, 2)
                if h == half:
                    wanted = jnp.where(q == row, slot + c, wanted)
            hit = jnp.where(line == wanted, 1.0, 0.0).astype(BF16)
            moved = nn(hit, both[:, half * part : (half + 1) * part])
            total = moved if total is None else total + moved
        total = total.astype(BF16)
        for d in range(count):
            out_ref[d, :, j * part : (j + 1) * part] = total[d * capp : (d + 1) * capp]


def backward(e, a, ra, b, rb, w, n_dp, n_ex, before=()):
    n, slot_count, half = a.shape
    width = w.shape[1]
    shape = (n_dp * n_ex, CAPP, width * CAP // CAPP) if before else (slot_count, width)
    return pl.pallas_call(
        functools.partial(backward_kernel, n_dp=n_dp),
        out_shape=[pltpu.VMEM((n, slot_count, 2 * half), BF16), pltpu.VMEM(shape, BF16)],
        in_specs=[pl.BlockSpec(memory_space=SMEM)]
        + [pl.BlockSpec(memory_space=VMEM)] * (5 + len(before)),
        out_specs=[pl.BlockSpec(memory_space=VMEM)] * 2,
        compiler_params=pltpu.CompilerParams(vmem_limit_bytes=LIMIT),
        name="backward",
    )(e, a, ra, b, rb, w, *before)


def weight_grad_kernel(*refs, planes, tile):
    x0_ref, x1_ref, g0_ref, g1_ref = refs[:4]
    out_ref, scratch, sem = refs[-3:]
    width = x0_ref.shape[2]
    copies = []
    for a in planes:
        x = jnp.concatenate([x0_ref[a // 2], x1_ref[a // 2]], axis=0)
        g = jnp.concatenate([g0_ref[a], g1_ref[a]], axis=0)
        for r in range(0, width, tile):
            i = len(copies)
            scratch[i] = tn(x[:, r : r + tile], g)
            copy = pltpu.make_async_copy(scratch.at[i], out_ref.at[a, pl.ds(r, tile)], sem.at[i])
            copy.start()
            copies.append(copy)
    for copy in copies:
        copy.wait()


def weight_grad(planes, x0, x1, g0, g1, total=None):
    n, _, cols = g0.shape
    width = x0.shape[2]
    tile = width // 3 if width % (3 * 128) == 0 else width
    steps = len(planes) * (width // tile)
    operands = [x0, x1, g0, g1] + ([] if total is None else [total])
    return pl.pallas_call(
        functools.partial(weight_grad_kernel, planes=planes, tile=tile),
        out_shape=pltpu.HBM((n, width, cols), F32),
        in_specs=[pl.BlockSpec(memory_space=VMEM)] * 4
        + [pl.BlockSpec(memory_space=pltpu.HBM)] * (len(operands) - 4),
        out_specs=pl.BlockSpec(memory_space=pltpu.HBM),
        scratch_shapes=[
            pltpu.VMEM((steps, tile, cols), F32),
            pltpu.SemaphoreType.DMA((steps,)),
        ],
        input_output_aliases={} if total is None else {4: 0},
        compiler_params=pltpu.CompilerParams(vmem_limit_bytes=LIMIT),
        name="weight_grad",
    )(*operands)


def place_kernel(hit_ref, got_ref, out_hbm, out_ref, sem, *, n_dp):
    copies = []
    count, capp, lanes = got_ref.shape
    n_ex = count // n_dp
    part = lanes // CAP
    hit = hit_ref[...]
    row = lax.broadcasted_iota(I32, (capp, hit.shape[1]), 0)
    picks = []
    for half in range(2):
        for j in range(CAP):
            pick = jnp.zeros(row.shape, F32)
            for r in range(capp):
                c, h = divmod(r * CAP + j, 2)
                if h == half:
                    pick = jnp.where(row == r, hit[c : c + 1], pick)
            picks.append(pick.astype(BF16))
    for p in range(n_dp):
        total = got_ref[p * n_ex].astype(F32)
        for e in range(1, n_ex):
            total = total + got_ref[p * n_ex + e].astype(F32)
        total = total.astype(BF16)
        for half in range(2):
            out = None
            for j in range(CAP):
                moved = tn(picks[half * CAP + j], total[:, j * part : (j + 1) * part])
                out = moved if out is None else out + moved
            at = (2 * p + half) * part
            out_ref[:, at : at + part] = out.astype(BF16)
        at = pl.ds(2 * p * part, 2 * part)
        copies.append(pltpu.make_async_copy(out_ref.at[:, at], out_hbm.at[:, at], sem.at[p]))
        copies[-1].start()
    for copy in copies:
        copy.wait()


def place(hit, got, tok, n_dp):
    width = got.shape[2] // CAP * 2
    return pl.pallas_call(
        functools.partial(place_kernel, n_dp=n_dp),
        out_shape=pltpu.HBM((tok, width * n_dp), BF16),
        in_specs=[pl.BlockSpec(memory_space=VMEM)] * 2,
        out_specs=pl.BlockSpec(memory_space=pltpu.HBM),
        scratch_shapes=[pltpu.VMEM((tok, width * n_dp), BF16), pltpu.SemaphoreType.DMA((n_dp,))],
        compiler_params=pltpu.CompilerParams(vmem_limit_bytes=LIMIT),
        name="place",
    )(hit, got)


def add_bf16(u, v):
    return (u.astype(F32) + v.astype(F32)).astype(BF16)


def shift(x, axis, k):
    return lax.ppermute(x, axis, xor_pairs(lax.axis_size(axis), k))


def pair_swap(x, phase):
    n_dp, n_ex = lax.axis_size("dp"), lax.axis_size("expert")
    pairs = []
    for d in range(n_dp):
        for ex in range(n_ex):
            k = 1 + ((ex & 1) ^ phase)
            pairs.append((d * n_ex + ex, (d ^ k) * n_ex + ex))
    return lax.ppermute(x, ("dp", "expert"), pairs)


def per_device_fast(out_grad, layer_input, expert_ids, gate_prob, w_stack, scale_exps):
    return fast_body(out_grad, layer_input, expert_ids, gate_prob, w_stack, scale_exps)


def fast_body(out_grad, layer_input, expert_ids, gate_prob, w_stack, scale_exps):
    n_dp = lax.axis_size("dp")
    n_ex = lax.axis_size("expert")
    n_z = n_ex // CORES
    tok = out_grad.shape[0]
    p = lax.axis_index("dp").astype(I32).reshape(1)
    e = lax.axis_index("expert").astype(I32).reshape(1)
    hit, *blocks = slots(p, e, expert_ids.T, gate_prob.T, out_grad, layer_input, n_dp)
    w = scale_weights(scale_exps, w_stack)
    got = [blocks[0]] + [shift(blocks[k], "dp", k) for k in range(1, n_dp)]
    mine = jnp.concatenate(got, axis=0)
    column = [mine] + [shift(mine, "expert", k * CORES) for k in range(1, n_z)]
    m0 = jnp.concatenate(column, axis=0)
    m1 = shift(m0, "expert", 1)
    xs, sums = [], []
    for m in (m0, m1):
        x, a, b = forward(p, m, w, n_dp, n_z)
        ra = pair_swap(a, 0)
        rb = pair_swap(b, 1)
        a = add_bf16(a, ra)
        b = add_bf16(b, rb)
        ra = pair_swap(a, 1)
        rb = pair_swap(b, 0)
        xs.append(x)
        sums.append((a, ra, b, rb))
    gs, out = [], ()
    for a, ra, b, rb in sums:
        g, *out = backward(e, a, ra, b, rb, w, n_dp, n_ex, out)
        gs.append(g)
    weight_grads = weight_grad((0, 1, 2), *xs, *gs)
    got = lax.all_to_all(out[0], ("dp", "expert"), split_axis=0, concat_axis=0, tiled=True)
    input_grad = place(hit, got, tok, n_dp)
    return input_grad, weight_grads


def per_device_any(out_grad, layer_input, expert_ids, gate_prob, w_stack, scale_exps):
    n_dp = lax.axis_size("dp")
    _, d_model = out_grad.shape
    routed = expert_ids == 0
    mask = jnp.any(routed, axis=1)
    prob = jnp.sum(jnp.where(routed, gate_prob, 0.0), axis=1)
    rank = jnp.cumsum(mask.astype(I32)) - 1
    hit = ((rank[None, :] == jnp.arange(CAP)[:, None]) & mask[None, :]).astype(BF16)
    slot_input = jnp.dot(hit, layer_input, preferred_element_type=F32)
    slot_prob = jnp.sum(hit.astype(F32) * prob[None, :], axis=1)
    slot_grad = slot_prob[:, None] * jnp.dot(hit, out_grad, preferred_element_type=F32)
    both = jnp.stack([slot_input, slot_grad]).astype(BF16)
    both = both.reshape(2, CAP, n_dp, d_model // n_dp).transpose(2, 0, 1, 3)
    both = lax.all_to_all(both, "dp", split_axis=0, concat_axis=0, tiled=True)
    both = lax.all_gather(both, "expert", axis=0)
    both = both.transpose(2, 0, 1, 3, 4)
    lead = both.shape[1:4]
    both = both.reshape(2, -1, both.shape[-1])
    n, rows, cols = w_stack.shape
    factor = jnp.exp2(scale_exps.astype(F32))
    tiles = factor.shape[1:]
    w = w_stack.astype(F32).reshape(n, tiles[0], rows // tiles[0], tiles[1], cols // tiles[1])
    w = (w * factor[:, :, None, :, None]).reshape(n, rows, cols).astype(BF16)
    sides = jnp.stack([both[0], both[0], both[1]])
    partial = jnp.einsum("nrk,nkh->nrh", sides, w, preferred_element_type=F32)
    gate, up, down = lax.psum(partial, "dp")
    sig = jax.nn.sigmoid(gate)
    act = gate * sig
    gate_grad = (down * up * sig * (1.0 + gate * (1.0 - sig))).astype(BF16)
    up_grad = (down * act).astype(BF16)
    hidden = (act * up).astype(BF16)
    back = nt(gate_grad, w[0]) + nt(up_grad, w[1])
    back = lax.psum_scatter(back.reshape(lead + (rows,)), "expert", scatter_dimension=0, tiled=False)
    back = lax.all_to_all(back, "dp", split_axis=0, concat_axis=0, tiled=True)
    back = back.transpose(1, 0, 2).reshape(CAP, d_model)
    input_grad = tn(hit, back.astype(BF16)).astype(BF16)
    weight_grads = jnp.einsum(
        "nrd,nrh->ndh", sides, jnp.stack([gate_grad, up_grad, hidden]), preferred_element_type=F32
    )
    return input_grad, weight_grads


def solution(mesh):
    n_dp, n_ex = mesh.shape["dp"], mesh.shape["expert"]
    n_z = n_ex // CORES
    fast = n_dp == 4 and n_ex % CORES == 0 and is_pow2(n_z) and n_z <= 4
    in_specs = (
        P(("dp", "expert"), None),
        P(("dp", "expert"), None),
        P(("dp", "expert"), None),
        P(("dp", "expert"), None),
        P(None, "dp", "expert"),
        P(None, "dp", "expert"),
    )
    out_specs = (P(("dp", "expert"), None), P(None, "dp", "expert"))
    return jax.shard_map(
        per_device_fast if fast else per_device_any,
        mesh=mesh,
        in_specs=in_specs,
        out_specs=out_specs,
        check_vma=False,
    )
```
